128 devices in a mesh: lat: 8 (over y, core), lon: 4 (over x), lev: 4 (over z).
Axes of the slice: x: 4, y: 4, z: 4, core: 2. Of those that a mesh axis runs over, the one named last changes fastest.
Arguments:
- tracer: float32 [32, 512, 128, 128], P('lat', 'lon', 'lev'), may hold values from 0.5 to 2
- conductance: float32 [32, 512, 128, 128], P('lat', 'lon', 'lev'), may hold values from 0.03 to 0.15
- source: float32 [32, 512, 128, 128], P('lat', 'lon', 'lev'), may hold values from -0.2 to 0.2
Outputs:
- standardized: float32 [32, 512, 128, 128], P('lat', 'lon', 'lev')
- tracer_end: float32 [32, 512, 128, 128], P('lat', 'lon', 'lev')
The draws below stay inside these ranges and needn't reach their ends.
All inputs are finite; a program needn't handle non-finite values.
Results may differ from the reference program's by a relative error of at most 0.00002.
Values sent between devices are 32-bit elements; how exact they have to be, the bound alone decides.
A program may use at most 128 MiB of HBM per device.

```python
import jax
import jax.numpy as jnp
from jax import lax

GRID_J = 32
GRID_I = 512
GRID_K = 128
MEMBERS = 128
STEPS = 3


def shard_levels(stream_key, extent, cuts, smallest, top_value):
    def one(dim, shards_of):
        draws = jax.random.uniform(jax.random.fold_in(jax.random.fold_in(stream_key, 6), dim), (shards_of,), jnp.float32, smallest / len(cuts), top_value / len(cuts))
        return jnp.repeat(jnp.exp(draws), extent[dim] // shards_of).reshape((-1,) + (1,) * (len(extent) - dim - 1))

    level = one(*cuts[0])
    for cut in cuts[1:]:
        level = level * one(*cut)
    return level


def setup_inputs(seed: int = 0) -> dict:
    seeds = jax.random.split(jax.random.key(seed), 4)
    return {
        "tracer": jnp.clip(0.5 + 1.5 * jax.random.uniform(seeds[0], (GRID_J, GRID_I, GRID_K, MEMBERS), jnp.float32) ** shard_levels(seeds[0], (GRID_J, GRID_I, GRID_K, MEMBERS), ((0, 8), (1, 4), (2, 4)), -0.2, 0.2), 0.5, 2.0),
        "conductance": jnp.clip(0.03 + 0.120000007 * jax.random.uniform(seeds[1], (GRID_J, GRID_I, GRID_K, MEMBERS), jnp.float32) ** shard_levels(seeds[1], (GRID_J, GRID_I, GRID_K, MEMBERS), ((0, 8), (1, 4), (2, 4)), -0.2, 0.2), 0.03, 0.15),
        "source": jnp.clip(jax.random.uniform(seeds[2], (GRID_J, GRID_I, GRID_K, MEMBERS), jnp.float32, -0.2, 0.2) * shard_levels(seeds[2], (GRID_J, GRID_I, GRID_K, MEMBERS), ((0, 8), (1, 4), (2, 4)), -0.4, 0.0), -0.2, 0.2),
    }


def inner_cells(values, dims):
    for dim in dims:
        values = lax.slice_in_dim(values, 1, values.shape[dim] - 1, axis=dim)
    return values

def side_cells(values, dim, start, dims):
    others = [other for other in dims if other != dim]
    values = inner_cells(values, others)
    return lax.slice_in_dim(values, start, start + values.shape[dim] - 2, axis=dim)

def advance(padded, conductance, source):
    middle = inner_cells(padded, (0, 1, 2))
    lower = [side_cells(padded, dim, 0, (0, 1, 2)) for dim in (0, 1, 2)]
    upper = [side_cells(padded, dim, 2, (0, 1, 2)) for dim in (0, 1, 2)]
    spread = lower[0] + upper[0] + lower[1] + upper[1] + lower[2] + upper[2] - 6.0 * middle
    return middle + conductance * spread + source

def reference(tracer, conductance, source):
    for step in range(STEPS):
        tracer = advance(jnp.pad(tracer, ((1, 1), (1, 1), (1, 1), (0, 0)), mode='constant'), conductance, source)
    line_mean = lax.optimization_barrier(jnp.mean(tracer, axis=1, keepdims=True))
    centred = tracer - line_mean
    line_variance = lax.optimization_barrier(jnp.mean(centred * centred, axis=1, keepdims=True))
    standardized = centred * lax.rsqrt(line_variance + 0.0001)
    return (standardized, tracer)
```

```python
import functools

import jax
import jax.numpy as jnp
from jax import lax
from jax.experimental import pallas as pl
from jax.experimental.pallas import tpu as pltpu
from jax.sharding import PartitionSpec as P

STEPS = 3
ROWS = 8
MESH = pl.DeviceIdType.MESH


def sweep(length, groups, total, centre, near, far, low, high, before, after, held, added, store, sums):
    row = lax.broadcasted_iota(jnp.int32, (ROWS, 128), 0)
    first, last = row == 0, row == ROWS - 1

    def block(t, carry, closing):
        previous, current, so_far = carry
        base = t * ROWS if closing else pl.multiple_of(t * ROWS, ROWS)
        lows = low(base) if 0 in groups else None
        highs = high(base) if total - 1 in groups else None
        for q in range(ROWS):
            i = base + q
            if closing and q == ROWS - 1:
                following = [after(g) for g in groups]
            else:
                following = [centre(i + 1, g) for g in groups]
            row_of = dict(zip(groups, current))
            for g in (groups[0] - 1, groups[-1] + 1):
                if 0 <= g < total:
                    row_of[g] = centre(i, g)
            down = {g: pltpu.roll(v, 1, 0) for g, v in row_of.items() if g <= groups[-1]}
            up = {g: pltpu.roll(v, ROWS - 1, 0) for g, v in row_of.items() if g >= groups[0]}
            if lows is not None:
                down[-1] = jnp.broadcast_to(lows[q : q + 1], (ROWS, 128))
            if highs is not None:
                up[total] = jnp.broadcast_to(highs[q : q + 1], (ROWS, 128))
            done = []
            for n, g in enumerate(groups):
                lower = jnp.where(first, down[g - 1], down[g])
                upper = jnp.where(last, up[g + 1], up[g])
                spread = (lower + upper) + (previous[n] + following[n]) + (near(i, g) + far(i, g))
                spread = spread - 6.0 * current[n]
                value = current[n] + held(i, g) * spread + added(i, g)
                store(i, g, value)
                done.append(value)
            if sums:
                so_far = [a + b for a, b in zip(so_far, done)]
            previous, current = current, following
        return previous, current, so_far

    zeros = [jnp.zeros((ROWS, 128), jnp.float32) for _ in groups] if sums else []
    carry = ([before(g) for g in groups], [centre(0, g) for g in groups], zeros)
    blocks = length // ROWS
    carry = lax.fori_loop(0, blocks - 1, lambda t, c: block(t, c, False), carry)
    return block(blocks - 1, carry, True)[2]


def along(length, body, carry, unroll=8):
    def block(t, carry):
        for q in range(unroll):
            carry = body(t * unroll + q, carry)
        return carry

    return lax.fori_loop(0, length // unroll, block, carry)


def march(
    sizes,
    tracer,
    conductance,
    source,
    end,
    scaled,
    even,
    odd,
    chip,
    pair,
    edge_k,
    edge_i,
    mine,
    theirs,
    mine_0,
    theirs_0,
    load_sem,
    chip_send,
    chip_recv,
    pair_send,
    pair_recv,
    k_send,
    k_recv,
    i_send,
    i_recv,
    sum_send,
    sum_recv,
    sum_0_send,
    sum_0_recv,
):
    n_lat, n_lon, n_lev = sizes
    planes, length, depth, _ = tracer.shape
    groups = list(range(depth // ROWS))
    total = len(groups)
    lat, lon, lev = (lax.axis_index(a) for a in ("lat", "lon", "lev"))
    core = lax.rem(lat, 2)
    way = 1 - 2 * core
    first = core * (planes - 1)
    rest = 1 - core
    partner = lat + way
    peer = lat - way
    has_peer = jnp.logical_and(peer >= 0, peer < n_lat)
    others = planes - 1

    def plane(p):
        return first + way * p

    def rows(g):
        return pl.ds(ROWS * g, ROWS)

    def load(n, p):
        a, b = ((tracer, even), (conductance, scaled), (source, end))[n]
        return pltpu.make_async_copy(a.at[plane(p)], b.at[plane(p)], load_sem.at[n, p])

    for n in range(3):
        for p in (*range(1, planes), 0):
            load(n, p).start()

    barrier = pltpu.get_barrier_semaphore()
    pl.semaphore_signal(barrier, 1, device_id={"lat": partner}, device_id_type=MESH)

    @pl.when(has_peer)
    def _():
        pl.semaphore_signal(barrier, 1, device_id={"lat": peer}, device_id_type=MESH)

    @pl.when(lev > 0)
    def _():
        pl.semaphore_signal(barrier, 1, device_id={"lev": lev - 1}, device_id_type=MESH)

    @pl.when(lev < n_lev - 1)
    def _():
        pl.semaphore_signal(barrier, 1, device_id={"lev": lev + 1}, device_id_type=MESH)

    for r in range(1, n_lon):
        pl.semaphore_signal(barrier, 1, device_id={"lon": lax.rem(lon + r, n_lon)}, device_id_type=MESH)
    pl.semaphore_wait(
        barrier,
        n_lon
        + has_peer.astype(jnp.int32)
        + (lev > 0).astype(jnp.int32)
        + (lev < n_lev - 1).astype(jnp.int32),
    )

    state = (even, odd, even)

    def chip_copy(s, g):
        origin = tracer if s == 0 else state[s]
        return pltpu.make_async_remote_copy(
            origin.at[plane(0), :, rows(g), :],
            chip.at[s, :, rows(g), :],
            chip_send.at[s, g],
            chip_recv.at[s, g],
            device_id={"lat": peer},
            device_id_type=MESH,
        )

    def pair_copy(s):
        origin = tracer if s == 0 else state[s]
        return pltpu.make_async_remote_copy(
            origin.at[plane(planes - 1)],
            pair.at[s],
            pair_send.at[s],
            pair_recv.at[s],
            device_id={"lat": partner},
            device_id_type=MESH,
        )

    def span(part):
        return pl.ds(rest, others) if part else pl.ds(first, 1)

    def k_copy(s, part, side):
        return pltpu.make_async_remote_copy(
            state[s].at[span(part), :, 0 if side else depth - 1, :],
            edge_k.at[s, side, span(part)],
            k_send.at[s, part, side],
            k_recv.at[s, part, side],
            device_id={"lev": lev - 1 if side else lev + 1},
            device_id_type=MESH,
        )

    def i_copy(s, part, side):
        return pltpu.make_async_remote_copy(
            state[s].at[span(part), 0 if side else length - 1],
            edge_i.at[s, side, span(part)],
            i_send.at[s, part, side],
            i_recv.at[s, part, side],
            device_id={"lon": lon - 1 if side else lon + 1},
            device_id_type=MESH,
        )

    def has(index, count, side):
        return index > 0 if side else index < count - 1

    def edges(action, s, part):
        for side in (0, 1):
            there = 1 - side if action == "wait_recv" else side

            @pl.when(has(lev, n_lev, there))
            def _(side=side):
                getattr(k_copy(s, part, side), action)()

            @pl.when(has(lon, n_lon, there))
            def _(side=side):
                getattr(i_copy(s, part, side), action)()

    @pl.when(has_peer)
    def _():
        for g in groups:
            chip_copy(0, g).start()

    pair_copy(0).start()

    def clear(ref, count):
        def one(i, _):
            ref[i] = jnp.zeros(ref.shape[1:], jnp.float32)
            return _

        lax.fori_loop(0, count, one, 0)

    @pl.when(jnp.logical_not(has_peer))
    def _():
        for s in range(STEPS):
            clear(chip.at[s], length)

    for side in (0, 1):

        @pl.when(jnp.logical_not(has(lev, n_lev, 1 - side)))
        def _(side=side):
            for s in range(STEPS):
                clear(edge_k.at[s, side], planes)

        @pl.when(jnp.logical_not(has(lon, n_lon, 1 - side)))
        def _(side=side):
            for s in range(STEPS):
                clear(edge_i.at[s, side], planes)

    def loader(ref, *lead):
        return lambda i, g: ref[(*lead, i, rows(g), slice(None))]

    def advance(s, p, which, near, far, sums=False):
        j = plane(p)
        target = end if s == STEPS - 1 else state[s + 1]

        def store(i, g, value):
            target[j, i, rows(g), :] = value

        return sweep(
            length,
            which,
            total,
            loader(state[s], j),
            near,
            far,
            lambda base: edge_k[s, 0, j, pl.ds(base, ROWS), :],
            lambda base: edge_k[s, 1, j, pl.ds(base, ROWS), :],
            lambda g: edge_i[s, 0, j, rows(g), :],
            lambda g: edge_i[s, 1, j, rows(g), :],
            loader(scaled, j),
            loader(end, j),
            store,
            sums,
        )

    def spread_of(j, which, sums):
        means = [v * (1.0 / length) for v in sums]

        def one(i, so_far):
            out = []
            for n, g in enumerate(which):
                d = end[j, i, rows(g), :] - means[n]
                out.append(so_far[n] + d * d)
            return out

        return means, along(length, one, [jnp.zeros((ROWS, 128), jnp.float32) for _ in which])

    def combined(own, arrived):
        means = [own[0], *(a[0] for a in arrived)]
        mean = functools.reduce(jnp.add, means) * (1.0 / n_lon)
        off = functools.reduce(jnp.add, [(m - mean) * (m - mean) for m in means])
        squares = functools.reduce(jnp.add, [own[1], *(a[1] for a in arrived)])
        variance = (squares + off * float(length)) * (1.0 / (length * n_lon))
        return mean, lax.rsqrt(variance + 0.0001)

    def scale(j, which, pairs):
        def one(i, carry):
            for g, (mean, factor) in zip(which, pairs):
                scaled[j, i, rows(g), :] = (end[j, i, rows(g), :] - mean) * factor
            return carry

        along(length, one, 0)

    def sum_copy(r):
        return pltpu.make_async_remote_copy(
            mine,
            theirs.at[r - 1],
            sum_send.at[r - 1],
            sum_recv.at[r - 1],
            device_id={"lon": lax.rem(lon + r, n_lon)},
            device_id_type=MESH,
        )

    def sum_0_copy(r, g):
        return pltpu.make_async_remote_copy(
            mine_0.at[g],
            theirs_0.at[r - 1, g],
            sum_0_send.at[r - 1, g],
            sum_0_recv.at[r - 1, g],
            device_id={"lon": lax.rem(lon + r, n_lon)},
            device_id_type=MESH,
        )

    for p in (*range(1, planes), 0):
        load(0, p).wait()
    for part in (1, 0):
        edges("start", 0, part)

    for s in range(STEPS):
        closing = s == STEPS - 1
        edges("wait_recv", s, 1)
        if s == 1:
            for part in (1, 0):
                edges("wait_send", 0, part)
        for p in range(1, planes):
            j = plane(p)
            if s == 0:
                load(1, p).wait()
                load(2, p).wait()
            if p == planes - 1:
                pair_copy(s).wait_recv()
                far = loader(pair, s)
            else:
                far = loader(state[s], plane(p + 1))
            sums = advance(s, p, groups, loader(state[s], plane(p - 1)), far, closing)
            if closing:
                means, squares = spread_of(j, groups, sums)
                for g in groups:
                    mine[0, p - 1, rows(g), :] = means[g]
                    mine[1, p - 1, rows(g), :] = squares[g]
        if closing:
            for r in range(1, n_lon):
                sum_copy(r).start()
            for r in range(1, n_lon):
                sum_copy(r).wait_recv()
            for p in range(1, planes):
                pairs = []
                for g in groups:
                    own = [mine[n, p - 1, rows(g), :] for n in (0, 1)]
                    rest_of = [[theirs[r, n, p - 1, rows(g), :] for n in (0, 1)] for r in range(n_lon - 1)]
                    pairs.append(combined(own, rest_of))
                scale(plane(p), groups, pairs)
        else:
            edges("start", s + 1, 1)
            pair_copy(s + 1).start()
        edges("wait_recv", s, 0)
        if s == 0:
            load(1, 0).wait()
            load(2, 0).wait()
        for g in groups:

            @pl.when(has_peer)
            def _(g=g):
                chip_copy(s, g).wait_recv()

            sums = advance(s, 0, [g], loader(chip, s), loader(state[s], plane(1)), closing)
            if closing:
                means, squares = spread_of(first, [g], sums)
                mine_0[g, 0] = means[0]
                mine_0[g, 1] = squares[0]
                for r in range(1, n_lon):
                    sum_0_copy(r, g).start()
                for r in range(1, n_lon):
                    sum_0_copy(r, g).wait_recv()
                arrived = [[theirs_0[r, g, n] for n in (0, 1)] for r in range(n_lon - 1)]
                scale(first, [g], [combined([means[0], squares[0]], arrived)])
            else:

                @pl.when(has_peer)
                def _(g=g):
                    chip_copy(s + 1, g).start()

        if not closing:
            edges("start", s + 1, 0)

    for s in range(STEPS):
        pair_copy(s).wait_send()

        @pl.when(has_peer)
        def _(s=s):
            for g in groups:
                chip_copy(s, g).wait_send()

        if s > 0:
            for part in (1, 0):
                edges("wait_send", s, part)
    for r in range(1, n_lon):
        sum_copy(r).wait_send()
        for g in groups:
            sum_0_copy(r, g).wait_send()


def hand_out(a, b, a_out, b_out, sem):
    copies = []
    for j in range(a.shape[0]):
        copies.append(pltpu.make_async_copy(a.at[j], a_out.at[j], sem.at[0, j]))
        copies.append(pltpu.make_async_copy(b.at[j], b_out.at[j], sem.at[1, j]))
    for c in copies:
        c.start()
    for c in copies:
        c.wait()


def shards(sizes, tracer, conductance, source):
    planes, length, depth, members = tracer.shape
    f32 = jnp.float32
    total = depth // ROWS
    lines = sizes[1] - 1
    dma = pltpu.SemaphoreType.DMA
    end, scaled = pl.pallas_call(
        functools.partial(march, sizes),
        out_shape=[pltpu.VMEM(tracer.shape, f32)] * 2,
        in_specs=[pl.BlockSpec(memory_space=pltpu.HBM)] * 3,
        out_specs=[pl.BlockSpec(memory_space=pltpu.VMEM)] * 2,
        scratch_shapes=[
            pltpu.VMEM(tracer.shape, f32),
            pltpu.VMEM(tracer.shape, f32),
            pltpu.VMEM((STEPS, length, depth, members), f32),
            pltpu.VMEM((STEPS, length, depth, members), f32),
            pltpu.VMEM((STEPS, 2, planes, length, members), f32),
            pltpu.VMEM((STEPS, 2, planes, depth, members), f32),
            pltpu.VMEM((2, planes - 1, depth, members), f32),
            pltpu.VMEM((lines, 2, planes - 1, depth, members), f32),
            pltpu.VMEM((total, 2, ROWS, members), f32),
            pltpu.VMEM((lines, total, 2, ROWS, members), f32),
            dma((3, planes)),
            dma((STEPS, total)),
            dma((STEPS, total)),
            dma((STEPS,)),
            dma((STEPS,)),
            dma((STEPS, 2, 2)),
            dma((STEPS, 2, 2)),
            dma((STEPS, 2, 2)),
            dma((STEPS, 2, 2)),
            dma((lines,)),
            dma((lines,)),
            dma((lines, total)),
            dma((lines, total)),
        ],
        compiler_params=pltpu.CompilerParams(
            collective_id=0, has_side_effects=True, vmem_limit_bytes=36 << 20
        ),
        name="march",
    )(tracer, conductance, source)
    scaled, end = pl.pallas_call(
        hand_out,
        out_shape=[jax.ShapeDtypeStruct(tracer.shape, f32)] * 2,
        in_specs=[pl.BlockSpec(memory_space=pltpu.VMEM)] * 2,
        out_specs=[pl.BlockSpec(memory_space=pltpu.HBM)] * 2,
        scratch_shapes=[dma((2, planes))],
        compiler_params=pltpu.CompilerParams(vmem_limit_bytes=1 << 20),
        name="hand_out",
    )(scaled, end)
    return scaled, end


def solution(mesh):
    sizes = tuple(mesh.shape[a] for a in ("lat", "lon", "lev"))
    placed = P("lat", "lon", "lev", None)
    return jax.shard_map(
        functools.partial(shards, sizes),
        mesh=mesh,
        in_specs=(placed,) * 3,
        out_specs=(placed, placed),
        check_vma=False,
    )
```

```python
import functools

import jax
import jax.numpy as jnp
from jax import lax
from jax.experimental import pallas as pl
from jax.experimental.pallas import tpu as pltpu
from jax.sharding import PartitionSpec as P

STEPS = 3
ROWS = 8
MESH = pl.DeviceIdType.MESH


def sweep(start, length, groups, total, centre, near, far, low, high, before, after, held, added, store, sums):
    row = lax.broadcasted_iota(jnp.int32, (ROWS, 128), 0)
    first, last = row == 0, row == ROWS - 1

    def block(t, carry, closing):
        previous, current, so_far = carry
        base = start + t * ROWS if closing else pl.multiple_of(start + t * ROWS, ROWS)
        lows = low(base) if 0 in groups else None
        highs = high(base) if total - 1 in groups else None
        for q in range(ROWS):
            i = base + q
            if closing and q == ROWS - 1:
                following = [after(g) for g in groups]
            else:
                following = [centre(i + 1, g) for g in groups]
            row_of = dict(zip(groups, current))
            for g in (groups[0] - 1, groups[-1] + 1):
                if 0 <= g < total:
                    row_of[g] = centre(i, g)
            down = {g: pltpu.roll(v, 1, 0) for g, v in row_of.items() if g <= groups[-1]}
            up = {g: pltpu.roll(v, ROWS - 1, 0) for g, v in row_of.items() if g >= groups[0]}
            if lows is not None:
                down[-1] = jnp.broadcast_to(lows[q : q + 1], (ROWS, 128))
            if highs is not None:
                up[total] = jnp.broadcast_to(highs[q : q + 1], (ROWS, 128))
            done = []
            for n, g in enumerate(groups):
                lower = jnp.where(first, down[g - 1], down[g])
                upper = jnp.where(last, up[g + 1], up[g])
                spread = (lower + upper) + (previous[n] + following[n]) + (near(i, g) + far(i, g))
                spread = spread - 6.0 * current[n]
                value = current[n] + held(i, g) * spread + added(i, g)
                store(i, g, value)
                done.append(value)
            if sums is not None:
                so_far = [a + b for a, b in zip(so_far, done)]
            previous, current = current, following
        return previous, current, so_far

    carry = ([before(g) for g in groups], [centre(start, g) for g in groups], sums or [])
    blocks = length // ROWS
    carry = lax.fori_loop(0, blocks - 1, lambda t, c: block(t, c, False), carry)
    return block(blocks - 1, carry, True)[2]


def along(length, body, carry, unroll=8):
    def block(t, carry):
        for q in range(unroll):
            carry = body(t * unroll + q, carry)
        return carry

    return lax.fori_loop(0, length // unroll, block, carry)


def march(
    sizes,
    tracer,
    conductance,
    source,
    end,
    scaled,
    even,
    odd,
    chip,
    pair,
    edge_k,
    edge_i,
    mine,
    theirs,
    mine_0,
    theirs_0,
    load_sem,
    chip_send,
    chip_recv,
    pair_send,
    pair_recv,
    k_send,
    k_recv,
    i_send,
    i_recv,
    sum_send,
    sum_recv,
    sum_0_send,
    sum_0_recv,
):
    n_lat, n_lon, n_lev = sizes
    planes, length, depth, _ = tracer.shape
    groups = list(range(depth // ROWS))
    total = len(groups)
    lat, lon, lev = (lax.axis_index(a) for a in ("lat", "lon", "lev"))
    core = lax.rem(lat, 2)
    way = 1 - 2 * core
    first = core * (planes - 1)
    rest = 1 - core
    partner = lat + way
    peer = lat - way
    has_peer = jnp.logical_and(peer >= 0, peer < n_lat)
    others = planes - 1

    def plane(p):
        return first + way * p

    def rows(g):
        return pl.ds(ROWS * g, ROWS)

    def load(n, p):
        a, b = ((tracer, even), (conductance, scaled), (source, end))[n]
        return pltpu.make_async_copy(a.at[plane(p)], b.at[plane(p)], load_sem.at[n, p])

    load(0, 0).start()

    barrier = pltpu.get_barrier_semaphore()
    signal = functools.partial(pl.semaphore_signal, barrier, 1, device_id_type=MESH)
    signal(device_id={"lat": partner})
    for r in range(1, n_lon):
        signal(device_id={"lon": lax.rem(lon + r, n_lon)})

    @pl.when(has_peer)
    def _():
        signal(device_id={"lat": peer})

    @pl.when(lev > 0)
    def _():
        signal(device_id={"lev": lev - 1})

    @pl.when(lev < n_lev - 1)
    def _():
        signal(device_id={"lev": lev + 1})

    pl.semaphore_wait(barrier, n_lon + sum(c.astype(jnp.int32) for c in (has_peer, lev > 0, lev < n_lev - 1)))

    state = (even, odd, even)

    def pieces(s, g):
        cuts = 4 if s == STEPS - 1 and g == total - 1 else 1
        return [(g + c, c * (length // cuts), length // cuts) for c in range(cuts)]

    def chip_copy(s, g, piece):
        number, start, count = piece
        return pltpu.make_async_remote_copy(
            state[s].at[first, pl.ds(start, count), rows(g), :],
            chip.at[s, pl.ds(start, count), rows(g), :],
            chip_send.at[s, number],
            chip_recv.at[s, number],
            device_id={"lat": peer},
            device_id_type=MESH,
        )

    def pair_copy(s):
        return pltpu.make_async_remote_copy(
            (tracer if s == 0 else state[s]).at[plane(planes - 1)],
            pair.at[s],
            pair_send.at[s],
            pair_recv.at[s],
            device_id={"lat": partner},
            device_id_type=MESH,
        )

    def span(part):
        return pl.ds(rest, others) if part else pl.ds(first, 1)

    def k_copy(s, part, side):
        return pltpu.make_async_remote_copy(
            state[s].at[span(part), :, 0 if side else depth - 1, :],
            edge_k.at[s, side, span(part)],
            k_send.at[s, part, side],
            k_recv.at[s, part, side],
            device_id={"lev": lev - 1 if side else lev + 1},
            device_id_type=MESH,
        )

    def i_copy(s, part, side):
        return pltpu.make_async_remote_copy(
            state[s].at[span(part), 0 if side else length - 1],
            edge_i.at[s, side, span(part)],
            i_send.at[s, part, side],
            i_recv.at[s, part, side],
            device_id={"lon": lon - 1 if side else lon + 1},
            device_id_type=MESH,
        )

    def has(index, count, side):
        return index > 0 if side else index < count - 1

    def edges(action, s, part):
        for side in (0, 1):
            there = 1 - side if action == "wait_recv" else side

            @pl.when(has(lev, n_lev, there))
            def _(side=side):
                getattr(k_copy(s, part, side), action)()

            @pl.when(has(lon, n_lon, there))
            def _(side=side):
                getattr(i_copy(s, part, side), action)()

    def chip_all(action, s, which):
        @pl.when(has_peer)
        def _():
            for g in which:
                for piece in pieces(s, g):
                    getattr(chip_copy(s, g, piece), action)()

    load(0, 0).wait()
    chip_all("start", 0, groups)
    pair_copy(0).start()
    for n in range(3):
        for p in (*range(1, planes), 0):
            if n or p:
                load(n, p).start()

    def clear(ref, count):
        def one(i, _):
            ref[i] = jnp.zeros(ref.shape[1:], jnp.float32)
            return _

        lax.fori_loop(0, count, one, 0)

    @pl.when(jnp.logical_not(has_peer))
    def _():
        for s in range(STEPS):
            clear(chip.at[s], length)

    for side in (0, 1):

        @pl.when(jnp.logical_not(has(lev, n_lev, 1 - side)))
        def _(side=side):
            for s in range(STEPS):
                clear(edge_k.at[s, side], planes)

        @pl.when(jnp.logical_not(has(lon, n_lon, 1 - side)))
        def _(side=side):
            for s in range(STEPS):
                clear(edge_i.at[s, side], planes)

    def loader(ref, *lead):
        return lambda i, g: ref[(*lead, i, rows(g), slice(None))]

    def advance(s, p, which, near, far, sums=None, start=0, count=length):
        j = plane(p)
        centre = loader(state[s], j)
        target = end if s == STEPS - 1 else state[s + 1]

        def store(i, g, value):
            target[j, i, rows(g), :] = value

        return sweep(
            start,
            count,
            which,
            total,
            centre,
            near,
            far,
            lambda base: edge_k[s, 0, j, pl.ds(base, ROWS), :],
            lambda base: edge_k[s, 1, j, pl.ds(base, ROWS), :],
            lambda g: centre(start - 1, g) if start else edge_i[s, 0, j, rows(g), :],
            lambda g: centre(start + count, g) if start + count < length else edge_i[s, 1, j, rows(g), :],
            loader(scaled, j),
            loader(end, j),
            store,
            sums,
        )

    def spread_of(j, which, sums, start, count):
        means = [v * (1.0 / count) for v in sums]

        def one(i, so_far):
            out = []
            for n, g in enumerate(which):
                d = end[j, start + i, rows(g), :] - means[n]
                out.append(so_far[n] + d * d)
            return out

        return means, along(count, one, nothing(which))

    def merged(one, other, start, count):
        (mean, squares), (mean_2, squares_2) = one, other
        off = mean_2 - mean
        share = count / (start + count)
        return mean + off * share, squares + squares_2 + off * off * (start * share)

    def combined(own, arrived):
        means = [own[0], *(a[0] for a in arrived)]
        mean = functools.reduce(jnp.add, means) * (1.0 / n_lon)
        off = functools.reduce(jnp.add, [(m - mean) * (m - mean) for m in means])
        squares = functools.reduce(jnp.add, [own[1], *(a[1] for a in arrived)])
        variance = (squares + off * float(length)) * (1.0 / (length * n_lon))
        return mean, lax.rsqrt(variance + 0.0001)

    def scale(j, which, pairs):
        def one(i, carry):
            for g, (mean, factor) in zip(which, pairs):
                scaled[j, i, rows(g), :] = (end[j, i, rows(g), :] - mean) * factor
            return carry

        along(length, one, 0)

    def sum_copy(r):
        return pltpu.make_async_remote_copy(
            mine,
            theirs.at[r - 1],
            sum_send.at[r - 1],
            sum_recv.at[r - 1],
            device_id={"lon": lax.rem(lon + r, n_lon)},
            device_id_type=MESH,
        )

    def sum_0_copy(r, g):
        return pltpu.make_async_remote_copy(
            mine_0.at[g],
            theirs_0.at[r - 1, g],
            sum_0_send.at[r - 1, g],
            sum_0_recv.at[r - 1, g],
            device_id={"lon": lax.rem(lon + r, n_lon)},
            device_id_type=MESH,
        )

    def nothing(which):
        return [jnp.zeros((ROWS, 128), jnp.float32) for _ in which]

    for p in range(1, planes):
        load(0, p).wait()
    for part in (1, 0):
        edges("start", 0, part)

    def scale_rest():
        for r in range(1, n_lon):
            sum_copy(r).wait_recv()
        for p in range(1, planes):
            pairs = []
            for g in groups:
                own = [mine[n, p - 1, rows(g), :] for n in (0, 1)]
                arrived = [[theirs[r, n, p - 1, rows(g), :] for n in (0, 1)] for r in range(n_lon - 1)]
                pairs.append(combined(own, arrived))
            scale(plane(p), groups, pairs)

    def scale_0(g):
        for r in range(1, n_lon):
            sum_0_copy(r, g).wait_recv()
        arrived = [[theirs_0[r, g, n] for n in (0, 1)] for r in range(n_lon - 1)]
        scale(first, [g], [combined([mine_0[g, n] for n in (0, 1)], arrived)])

    for s in range(STEPS):
        closing = s == STEPS - 1
        edges("wait_recv", s, 1)
        if s == 1:
            pair_copy(0).wait_send()
            for part in (1, 0):
                edges("wait_send", 0, part)
        for p in range(1, planes):
            j = plane(p)
            if s == 0:
                load(1, p).wait()
                load(2, p).wait()
            if p == planes - 1:
                pair_copy(s).wait_recv()
                far = loader(pair, s)
            else:
                far = loader(state[s], plane(p + 1))
            sums = advance(s, p, groups, loader(state[s], plane(p - 1)), far, nothing(groups) if closing else None)
            if closing:
                means, squares = spread_of(j, groups, sums, 0, length)
                for g in groups:
                    mine[0, p - 1, rows(g), :] = means[g]
                    mine[1, p - 1, rows(g), :] = squares[g]
        if closing:
            for r in range(1, n_lon):
                sum_copy(r).start()
        else:
            edges("start", s + 1, 1)
            pair_copy(s + 1).start()
        edges("wait_recv", s, 0)
        if s == 0:
            load(1, 0).wait()
            load(2, 0).wait()
        for g in groups:
            if s == 1:
                chip_all("wait_send", 0, [g])
            for piece in pieces(s, g):
                _, start, count = piece

                @pl.when(has_peer)
                def _(g=g, piece=piece):
                    chip_copy(s, g, piece).wait_recv()

                near, far = loader(chip, s), loader(state[s], plane(1))
                sums = advance(s, 0, [g], near, far, nothing([g]) if closing else None, start, count)
                if closing:
                    (mean,), (squares,) = spread_of(first, [g], sums, start, count)
                    line = merged(line, (mean, squares), start, count) if start else (mean, squares)
                if closing and g == total - 1 and start == 0:
                    scale_0(g - 1)
            if closing:
                for n in (0, 1):
                    mine_0[g, n] = line[n]
                for r in range(1, n_lon):
                    sum_0_copy(r, g).start()
                if g == 0:
                    scale_rest()
                elif g < total - 1:
                    scale_0(g - 1)
                else:
                    scale_0(g)
            else:
                chip_all("start", s + 1, [g])
        if not closing:
            edges("start", s + 1, 0)

    for s in range(1, STEPS):
        pair_copy(s).wait_send()
        chip_all("wait_send", s, groups)
        for part in (1, 0):
            edges("wait_send", s, part)
    for r in range(1, n_lon):
        sum_copy(r).wait_send()
        for g in groups:
            sum_0_copy(r, g).wait_send()


def hand_out(a, b, a_out, b_out, sem):
    copies = []
    for j in range(a.shape[0]):
        copies.append(pltpu.make_async_copy(a.at[j], a_out.at[j], sem.at[0, j]))
        copies.append(pltpu.make_async_copy(b.at[j], b_out.at[j], sem.at[1, j]))
    for c in copies:
        c.start()
    for c in copies:
        c.wait()


def shards(sizes, tracer, conductance, source):
    planes, length, depth, members = tracer.shape
    f32 = jnp.float32
    total = depth // ROWS
    lines = sizes[1] - 1
    dma = pltpu.SemaphoreType.DMA
    end, scaled = pl.pallas_call(
        functools.partial(march, sizes),
        out_shape=[pltpu.VMEM(tracer.shape, f32)] * 2,
        in_specs=[pl.BlockSpec(memory_space=pltpu.HBM)] * 3,
        out_specs=[pl.BlockSpec(memory_space=pltpu.VMEM)] * 2,
        scratch_shapes=[
            pltpu.VMEM(tracer.shape, f32),
            pltpu.VMEM(tracer.shape, f32),
            pltpu.VMEM((STEPS, length, depth, members), f32),
            pltpu.VMEM((STEPS, length, depth, members), f32),
            pltpu.VMEM((STEPS, 2, planes, length, members), f32),
            pltpu.VMEM((STEPS, 2, planes, depth, members), f32),
            pltpu.VMEM((2, planes - 1, depth, members), f32),
            pltpu.VMEM((lines, 2, planes - 1, depth, members), f32),
            pltpu.VMEM((total, 2, ROWS, members), f32),
            pltpu.VMEM((lines, total, 2, ROWS, members), f32),
            dma((3, planes)),
            dma((STEPS, total + 3)),
            dma((STEPS, total + 3)),
            dma((STEPS,)),
            dma((STEPS,)),
            dma((STEPS, 2, 2)),
            dma((STEPS, 2, 2)),
            dma((STEPS, 2, 2)),
            dma((STEPS, 2, 2)),
            dma((lines,)),
            dma((lines,)),
            dma((lines, total)),
            dma((lines, total)),
        ],
        compiler_params=pltpu.CompilerParams(
            collective_id=0, has_side_effects=True, vmem_limit_bytes=36 << 20
        ),
        name="march",
    )(tracer, conductance, source)
    scaled, end = pl.pallas_call(
        hand_out,
        out_shape=[jax.ShapeDtypeStruct(tracer.shape, f32)] * 2,
        in_specs=[pl.BlockSpec(memory_space=pltpu.VMEM)] * 2,
        out_specs=[pl.BlockSpec(memory_space=pltpu.HBM)] * 2,
        scratch_shapes=[dma((2, planes))],
        compiler_params=pltpu.CompilerParams(vmem_limit_bytes=1 << 20),
        name="hand_out",
    )(scaled, end)
    return scaled, end


def solution(mesh):
    sizes = tuple(mesh.shape[a] for a in ("lat", "lon", "lev"))
    placed = P("lat", "lon", "lev", None)
    return jax.shard_map(
        functools.partial(shards, sizes),
        mesh=mesh,
        in_specs=(placed,) * 3,
        out_specs=(placed, placed),
        check_vma=False,
    )
```

```python
import functools

import jax
import jax.numpy as jnp
from jax import lax
from jax.experimental import pallas as pl
from jax.experimental.pallas import tpu as pltpu
from jax.sharding import PartitionSpec as P

STEPS = 3
ROWS = 8
MESH = pl.DeviceIdType.MESH


def sweep(start, length, groups, total, centre, near, far, low, high, before, after, held, added, store, sums):
    row = lax.broadcasted_iota(jnp.int32, (ROWS, 128), 0)
    first, last = row == 0, row == ROWS - 1

    def block(t, carry, closing):
        previous, current, so_far = carry
        base = start + t * ROWS if closing else pl.multiple_of(start + t * ROWS, ROWS)
        lows = low(base) if 0 in groups else None
        highs = high(base) if total - 1 in groups else None
        for q in range(ROWS):
            i = base + q
            if closing and q == ROWS - 1:
                following = [after(g) for g in groups]
            else:
                following = [centre(i + 1, g) for g in groups]
            row_of = dict(zip(groups, current))
            for g in (groups[0] - 1, groups[-1] + 1):
                if 0 <= g < total:
                    row_of[g] = centre(i, g)
            down = {g: pltpu.roll(v, 1, 0) for g, v in row_of.items() if g <= groups[-1]}
            up = {g: pltpu.roll(v, ROWS - 1, 0) for g, v in row_of.items() if g >= groups[0]}
            if lows is not None:
                down[-1] = jnp.broadcast_to(lows[q : q + 1], (ROWS, 128))
            if highs is not None:
                up[total] = jnp.broadcast_to(highs[q : q + 1], (ROWS, 128))
            done = []
            for n, g in enumerate(groups):
                lower = jnp.where(first, down[g - 1], down[g])
                upper = jnp.where(last, up[g + 1], up[g])
                spread = (lower + upper) + (previous[n] + following[n]) + (near(i, g) + far(i, g))
                spread = spread - 6.0 * current[n]
                value = current[n] + held(i, g) * spread + added(i, g)
                store(i, g, value)
                done.append(value)
            if sums is not None:
                so_far = [a + b for a, b in zip(so_far, done)]
            previous, current = current, following
        return previous, current, so_far

    carry = ([before(g) for g in groups], [centre(start, g) for g in groups], sums or [])
    blocks = length // ROWS
    carry = lax.fori_loop(0, blocks - 1, lambda t, c: block(t, c, False), carry)
    return block(blocks - 1, carry, True)[2]


def along(length, body, carry, unroll=8):
    def block(t, carry):
        for q in range(unroll):
            carry = body(t * unroll + q, carry)
        return carry

    return lax.fori_loop(0, length // unroll, block, carry)


def march(
    sizes,
    tracer,
    conductance,
    source,
    end,
    scaled,
    even,
    odd,
    chip,
    pair,
    edge_k,
    edge_i,
    mine,
    theirs,
    mine_0,
    theirs_0,
    gather,
    across,
    go,
    load_sem,
    first_sem,
    chip_send,
    chip_recv,
    pair_send,
    pair_recv,
    k_send,
    k_recv,
    i_send,
    i_recv,
    sum_send,
    sum_recv,
    sum_0_send,
    sum_0_recv,
):
    n_lat, n_lon, n_lev = sizes
    planes, length, depth, _ = tracer.shape
    groups = list(range(depth // ROWS))
    total = len(groups)
    lat, lon, lev = (lax.axis_index(a) for a in ("lat", "lon", "lev"))
    core = lax.rem(lat, 2)
    way = 1 - 2 * core
    first = core * (planes - 1)
    rest = 1 - core
    partner = lat + way
    peer = lat - way
    has_peer = jnp.logical_and(peer >= 0, peer < n_lat)
    others = planes - 1

    def plane(p):
        return first + way * p

    def rows(g):
        return pl.ds(ROWS * g, ROWS)

    def load(n, p):
        a, b = ((tracer, even), (conductance, scaled), (source, end))[n]
        return pltpu.make_async_copy(a.at[plane(p)], b.at[plane(p)], load_sem.at[n, p])

    def load_first(g):
        return pltpu.make_async_copy(
            tracer.at[first, :, rows(g), :], even.at[first, :, rows(g), :], first_sem.at[g]
        )

    for g in groups:
        load_first(g).start()

    barrier = pltpu.get_barrier_semaphore()
    signal = functools.partial(pl.semaphore_signal, inc=1, device_id_type=MESH)

    def greet(semaphore):
        for r in range(1, n_lon):
            signal(semaphore, device_id={"lon": lax.rem(lon + r, n_lon)})

        @pl.when(lev > 0)
        def _():
            signal(semaphore, device_id={"lev": lev - 1})

        @pl.when(lev < n_lev - 1)
        def _():
            signal(semaphore, device_id={"lev": lev + 1})

    beside = n_lon - 1 + (lev > 0).astype(jnp.int32) + (lev < n_lev - 1).astype(jnp.int32)
    signal(barrier, device_id={"lat": partner})

    @pl.when(has_peer)
    def _():
        signal(barrier, device_id={"lat": peer})

    @pl.when(jnp.logical_not(has_peer))
    def _():
        greet(barrier)

    pl.semaphore_wait(barrier, jnp.where(has_peer, 2, 1 + beside))

    state = (even, odd, even)

    def pieces(s, g):
        cuts = 4 if s == STEPS - 1 and g == total - 1 else 1
        return [(g + c, c * (length // cuts), length // cuts) for c in range(cuts)]

    def chip_copy(s, g, piece):
        number, start, count = piece
        return pltpu.make_async_remote_copy(
            state[s].at[first, pl.ds(start, count), rows(g), :],
            chip.at[s, pl.ds(start, count), rows(g), :],
            chip_send.at[s, number],
            chip_recv.at[s, number],
            device_id={"lat": peer},
            device_id_type=MESH,
        )

    def pair_copy(s):
        return pltpu.make_async_remote_copy(
            (tracer if s == 0 else state[s]).at[plane(planes - 1)],
            pair.at[s],
            pair_send.at[s],
            pair_recv.at[s],
            device_id={"lat": partner},
            device_id_type=MESH,
        )

    def span(part):
        return pl.ds(rest, others) if part else pl.ds(first, 1)

    def k_copy(s, part, side):
        return pltpu.make_async_remote_copy(
            state[s].at[span(part), :, 0 if side else depth - 1, :],
            edge_k.at[s, side, span(part)],
            k_send.at[s, part, side],
            k_recv.at[s, part, side],
            device_id={"lev": lev - 1 if side else lev + 1},
            device_id_type=MESH,
        )

    def i_copy(s, part, side):
        return pltpu.make_async_remote_copy(
            state[s].at[span(part), 0 if side else length - 1],
            edge_i.at[s, side, span(part)],
            i_send.at[s, part, side],
            i_recv.at[s, part, side],
            device_id={"lon": lon - 1 if side else lon + 1},
            device_id_type=MESH,
        )

    def has(index, count, side):
        return index > 0 if side else index < count - 1

    def edges(action, s, part):
        for side in (0, 1):
            there = 1 - side if action == "wait_recv" else side

            @pl.when(has(lev, n_lev, there))
            def _(side=side):
                getattr(k_copy(s, part, side), action)()

            @pl.when(has(lon, n_lon, there))
            def _(side=side):
                getattr(i_copy(s, part, side), action)()

    def chip_all(action, s, which):
        @pl.when(has_peer)
        def _():
            for g in which:
                for piece in pieces(s, g):
                    getattr(chip_copy(s, g, piece), action)()

    for g in groups:
        load_first(g).wait()
        chip_all("start", 0, [g])
    pair_copy(0).start()
    for n in range(3):
        for p in (*range(1, planes), 0):
            if n or p:
                load(n, p).start()

    def clear(ref, count):
        def one(i, _):
            ref[i] = jnp.zeros(ref.shape[1:], jnp.float32)
            return _

        lax.fori_loop(0, count, one, 0)

    @pl.when(jnp.logical_not(has_peer))
    def _():
        for s in range(STEPS):
            clear(chip.at[s], length)

    for side in (0, 1):

        @pl.when(jnp.logical_not(has(lev, n_lev, 1 - side)))
        def _(side=side):
            for s in range(STEPS):
                clear(edge_k.at[s, side], planes)

        @pl.when(jnp.logical_not(has(lon, n_lon, 1 - side)))
        def _(side=side):
            for s in range(STEPS):
                clear(edge_i.at[s, side], planes)

    half = n_lat // 2
    low_half = lat < half
    depth_in = jnp.where(low_half, lat, n_lat - 1 - lat)
    inward = jnp.where(low_half, lat + 1, lat - 1)
    outward = jnp.where(low_half, lat - 1, lat + 1)

    @pl.when(depth_in < half - 1)
    def _():
        pl.semaphore_wait(gather, 1)

    @pl.when(depth_in > 0)
    def _():
        signal(gather, device_id={"lat": outward})
        pl.semaphore_wait(go, 1)

    @pl.when(depth_in == 0)
    def _():
        greet(across)
        pl.semaphore_wait(across, beside)

    @pl.when(depth_in < half - 1)
    def _():
        signal(go, device_id={"lat": inward})

    def loader(ref, *lead):
        return lambda i, g: ref[(*lead, i, rows(g), slice(None))]

    def advance(s, p, which, near, far, sums=None, start=0, count=length):
        j = plane(p)
        centre = loader(state[s], j)
        target = end if s == STEPS - 1 else state[s + 1]

        def store(i, g, value):
            target[j, i, rows(g), :] = value

        return sweep(
            start,
            count,
            which,
            total,
            centre,
            near,
            far,
            lambda base: edge_k[s, 0, j, pl.ds(base, ROWS), :],
            lambda base: edge_k[s, 1, j, pl.ds(base, ROWS), :],
            lambda g: centre(start - 1, g) if start else edge_i[s, 0, j, rows(g), :],
            lambda g: centre(start + count, g) if start + count < length else edge_i[s, 1, j, rows(g), :],
            loader(scaled, j),
            loader(end, j),
            store,
            sums,
        )

    def spread_of(j, which, sums, start, count):
        means = [v * (1.0 / count) for v in sums]

        def one(i, so_far):
            out = []
            for n, g in enumerate(which):
                d = end[j, start + i, rows(g), :] - means[n]
                out.append(so_far[n] + d * d)
            return out

        return means, along(count, one, nothing(which))

    def merged(one, other, start, count):
        (mean, squares), (mean_2, squares_2) = one, other
        off = mean_2 - mean
        share = count / (start + count)
        return mean + off * share, squares + squares_2 + off * off * (start * share)

    def combined(own, arrived):
        means = [own[0], *(a[0] for a in arrived)]
        mean = functools.reduce(jnp.add, means) * (1.0 / n_lon)
        off = functools.reduce(jnp.add, [(m - mean) * (m - mean) for m in means])
        squares = functools.reduce(jnp.add, [own[1], *(a[1] for a in arrived)])
        variance = (squares + off * float(length)) * (1.0 / (length * n_lon))
        return mean, lax.rsqrt(variance + 0.0001)

    def scale(j, which, pairs):
        def one(i, carry):
            for g, (mean, factor) in zip(which, pairs):
                scaled[j, i, rows(g), :] = (end[j, i, rows(g), :] - mean) * factor
            return carry

        along(length, one, 0)

    def sum_copy(r):
        return pltpu.make_async_remote_copy(
            mine,
            theirs.at[r - 1],
            sum_send.at[r - 1],
            sum_recv.at[r - 1],
            device_id={"lon": lax.rem(lon + r, n_lon)},
            device_id_type=MESH,
        )

    def sum_0_copy(r, g):
        return pltpu.make_async_remote_copy(
            mine_0.at[g],
            theirs_0.at[r - 1, g],
            sum_0_send.at[r - 1, g],
            sum_0_recv.at[r - 1, g],
            device_id={"lon": lax.rem(lon + r, n_lon)},
            device_id_type=MESH,
        )

    def nothing(which):
        return [jnp.zeros((ROWS, 128), jnp.float32) for _ in which]

    for p in range(1, planes):
        load(0, p).wait()
    for part in (1, 0):
        edges("start", 0, part)

    def scale_rest():
        for r in range(1, n_lon):
            sum_copy(r).wait_recv()
        for p in range(1, planes):
            pairs = []
            for g in groups:
                own = [mine[n, p - 1, rows(g), :] for n in (0, 1)]
                arrived = [[theirs[r, n, p - 1, rows(g), :] for n in (0, 1)] for r in range(n_lon - 1)]
                pairs.append(combined(own, arrived))
            scale(plane(p), groups, pairs)

    def scale_0(g):
        for r in range(1, n_lon):
            sum_0_copy(r, g).wait_recv()
        arrived = [[theirs_0[r, g, n] for n in (0, 1)] for r in range(n_lon - 1)]
        scale(first, [g], [combined([mine_0[g, n] for n in (0, 1)], arrived)])

    for s in range(STEPS):
        closing = s == STEPS - 1
        edges("wait_recv", s, 1)
        if s == 1:
            pair_copy(0).wait_send()
            for part in (1, 0):
                edges("wait_send", 0, part)
        for p in range(1, planes):
            j = plane(p)
            if s == 0:
                load(1, p).wait()
                load(2, p).wait()
            if p == planes - 1:
                pair_copy(s).wait_recv()
                far = loader(pair, s)
            else:
                far = loader(state[s], plane(p + 1))
            sums = advance(s, p, groups, loader(state[s], plane(p - 1)), far, nothing(groups) if closing else None)
            if closing:
                means, squares = spread_of(j, groups, sums, 0, length)
                for g in groups:
                    mine[0, p - 1, rows(g), :] = means[g]
                    mine[1, p - 1, rows(g), :] = squares[g]
        if closing:
            for r in range(1, n_lon):
                sum_copy(r).start()
        else:
            edges("start", s + 1, 1)
            pair_copy(s + 1).start()
        edges("wait_recv", s, 0)
        if s == 0:
            load(1, 0).wait()
            load(2, 0).wait()
        for g in groups:
            if s == 1:
                chip_all("wait_send", 0, [g])
            for piece in pieces(s, g):
                _, start, count = piece

                @pl.when(has_peer)
                def _(g=g, piece=piece):
                    chip_copy(s, g, piece).wait_recv()

                near, far = loader(chip, s), loader(state[s], plane(1))
                sums = advance(s, 0, [g], near, far, nothing([g]) if closing else None, start, count)
                if closing:
                    (mean,), (squares,) = spread_of(first, [g], sums, start, count)
                    line = merged(line, (mean, squares), start, count) if start else (mean, squares)
                if closing and g == total - 1 and start == 0:
                    scale_0(g - 1)
            if closing:
                for n in (0, 1):
                    mine_0[g, n] = line[n]
                for r in (*range(2, n_lon), 1):
                    sum_0_copy(r, g).start()
                if g == 0:
                    scale_rest()
                elif g < total - 1:
                    scale_0(g - 1)
                else:
                    scale_0(g)
            else:
                chip_all("start", s + 1, [g])
        if not closing:
            edges("start", s + 1, 0)

    for s in range(1, STEPS):
        pair_copy(s).wait_send()
        chip_all("wait_send", s, groups)
        for part in (1, 0):
            edges("wait_send", s, part)
    for r in range(1, n_lon):
        sum_copy(r).wait_send()
        for g in groups:
            sum_0_copy(r, g).wait_send()


def hand_out(a, b, a_out, b_out, sem):
    copies = []
    for j in range(a.shape[0]):
        copies.append(pltpu.make_async_copy(a.at[j], a_out.at[j], sem.at[0, j]))
        copies.append(pltpu.make_async_copy(b.at[j], b_out.at[j], sem.at[1, j]))
    for c in copies:
        c.start()
    for c in copies:
        c.wait()


def shards(sizes, tracer, conductance, source):
    planes, length, depth, members = tracer.shape
    f32 = jnp.float32
    total = depth // ROWS
    lines = sizes[1] - 1
    dma = pltpu.SemaphoreType.DMA
    end, scaled = pl.pallas_call(
        functools.partial(march, sizes),
        out_shape=[pltpu.VMEM(tracer.shape, f32)] * 2,
        in_specs=[pl.BlockSpec(memory_space=pltpu.HBM)] * 3,
        out_specs=[pl.BlockSpec(memory_space=pltpu.VMEM)] * 2,
        scratch_shapes=[
            pltpu.VMEM(tracer.shape, f32),
            pltpu.VMEM(tracer.shape, f32),
            pltpu.VMEM((STEPS, length, depth, members), f32),
            pltpu.VMEM((STEPS, length, depth, members), f32),
            pltpu.VMEM((STEPS, 2, planes, length, members), f32),
            pltpu.VMEM((STEPS, 2, planes, depth, members), f32),
            pltpu.VMEM((2, planes - 1, depth, members), f32),
            pltpu.VMEM((lines, 2, planes - 1, depth, members), f32),
            pltpu.VMEM((total, 2, ROWS, members), f32),
            pltpu.VMEM((lines, total, 2, ROWS, members), f32),
            pltpu.SemaphoreType.REGULAR,
            pltpu.SemaphoreType.REGULAR,
            pltpu.SemaphoreType.REGULAR,
            dma((3, planes)),
            dma((total,)),
            dma((STEPS, total + 3)),
            dma((STEPS, total + 3)),
            dma((STEPS,)),
            dma((STEPS,)),
            dma((STEPS, 2, 2)),
            dma((STEPS, 2, 2)),
            dma((STEPS, 2, 2)),
            dma((STEPS, 2, 2)),
            dma((lines,)),
            dma((lines,)),
            dma((lines, total)),
            dma((lines, total)),
        ],
        compiler_params=pltpu.CompilerParams(
            collective_id=0, has_side_effects=True, vmem_limit_bytes=36 << 20
        ),
        name="march",
    )(tracer, conductance, source)
    scaled, end = pl.pallas_call(
        hand_out,
        out_shape=[jax.ShapeDtypeStruct(tracer.shape, f32)] * 2,
        in_specs=[pl.BlockSpec(memory_space=pltpu.VMEM)] * 2,
        out_specs=[pl.BlockSpec(memory_space=pltpu.HBM)] * 2,
        scratch_shapes=[dma((2, planes))],
        compiler_params=pltpu.CompilerParams(vmem_limit_bytes=1 << 20),
        name="hand_out",
    )(scaled, end)
    return scaled, end


def solution(mesh):
    sizes = tuple(mesh.shape[a] for a in ("lat", "lon", "lev"))
    placed = P("lat", "lon", "lev", None)
    return jax.shard_map(
        functools.partial(shards, sizes),
        mesh=mesh,
        in_specs=(placed,) * 3,
        out_specs=(placed, placed),
        check_vma=False,
    )
```

```python
import functools

import jax
import jax.numpy as jnp
from jax import lax
from jax.experimental import pallas as pl
from jax.experimental.pallas import tpu as pltpu
from jax.sharding import PartitionSpec as P

STEPS = 3
ROWS = 8
MESH = pl.DeviceIdType.MESH


def sweep(start, length, groups, total, centre, near, far, low, high, before, after, held, added, store, sums):
    row = lax.broadcasted_iota(jnp.int32, (ROWS, 128), 0)
    first, last = row == 0, row == ROWS - 1

    def block(t, carry, closing):
        previous, current, so_far = carry
        base = start + t * ROWS if closing else pl.multiple_of(start + t * ROWS, ROWS)
        lows = low(base) if 0 in groups else None
        highs = high(base) if total - 1 in groups else None
        for q in range(ROWS):
            i = base + q
            if closing and q == ROWS - 1:
                following = [after(g) for g in groups]
            else:
                following = [centre(i + 1, g) for g in groups]
            row_of = dict(zip(groups, current))
            for g in (groups[0] - 1, groups[-1] + 1):
                if 0 <= g < total:
                    row_of[g] = centre(i, g)
            down = {g: pltpu.roll(v, 1, 0) for g, v in row_of.items() if g <= groups[-1]}
            up = {g: pltpu.roll(v, ROWS - 1, 0) for g, v in row_of.items() if g >= groups[0]}
            if lows is not None:
                down[-1] = jnp.broadcast_to(lows[q : q + 1], (ROWS, 128))
            if highs is not None:
                up[total] = jnp.broadcast_to(highs[q : q + 1], (ROWS, 128))
            done = []
            for n, g in enumerate(groups):
                lower = jnp.where(first, down[g - 1], down[g])
                upper = jnp.where(last, up[g + 1], up[g])
                spread = (lower + upper) + (previous[n] + following[n]) + (near(i, g) + far(i, g))
                spread = spread - 6.0 * current[n]
                value = current[n] + held(i, g) * spread + added(i, g)
                store(i, g, value)
                done.append(value)
            if sums is not None:
                so_far = [a + b for a, b in zip(so_far, done)]
            previous, current = current, following
        return previous, current, so_far

    carry = ([before(g) for g in groups], [centre(start, g) for g in groups], sums or [])
    blocks = length // ROWS
    carry = lax.fori_loop(0, blocks - 1, lambda t, c: block(t, c, False), carry)
    return block(blocks - 1, carry, True)[2]


def along(length, body, carry, unroll=8):
    def block(t, carry):
        for q in range(unroll):
            carry = body(t * unroll + q, carry)
        return carry

    return lax.fori_loop(0, length // unroll, block, carry)


def march(
    sizes,
    tracer,
    conductance,
    source,
    end,
    scaled,
    closing_line,
    even,
    odd,
    chip,
    pair,
    edge_k,
    edge_i,
    mine,
    theirs,
    mine_0,
    theirs_0,
    gather,
    across,
    go,
    load_sem,
    chip_send,
    chip_recv,
    pair_send,
    pair_recv,
    k_send,
    k_recv,
    i_send,
    i_recv,
    sum_send,
    sum_recv,
    sum_0_send,
    sum_0_recv,
):
    n_lat, n_lon, n_lev = sizes
    planes, length, depth, _ = tracer.shape
    groups = list(range(depth // ROWS))
    total = len(groups)
    lat, lon, lev = (lax.axis_index(a) for a in ("lat", "lon", "lev"))
    core = lax.rem(lat, 2)
    way = 1 - 2 * core
    first = core * (planes - 1)
    rest = 1 - core
    partner = lat + way
    peer = lat - way
    has_peer = jnp.logical_and(peer >= 0, peer < n_lat)
    others = planes - 1

    def plane(p):
        return first + way * p

    def rows(g):
        return pl.ds(ROWS * g, ROWS)

    def load(n, p):
        a, b = ((tracer, even), (conductance, scaled), (source, end))[n]
        return pltpu.make_async_copy(a.at[plane(p)], b.at[plane(p)], load_sem.at[n, p])


    barrier = pltpu.get_barrier_semaphore()
    signal = functools.partial(pl.semaphore_signal, inc=1, device_id_type=MESH)

    def greet(semaphore):
        for r in range(1, n_lon):
            signal(semaphore, device_id={"lon": lax.rem(lon + r, n_lon)})

        @pl.when(lev > 0)
        def _():
            signal(semaphore, device_id={"lev": lev - 1})

        @pl.when(lev < n_lev - 1)
        def _():
            signal(semaphore, device_id={"lev": lev + 1})

    beside = n_lon - 1 + (lev > 0).astype(jnp.int32) + (lev < n_lev - 1).astype(jnp.int32)

    @pl.when(has_peer)
    def _():
        signal(barrier, device_id={"lat": peer})

    signal(barrier, device_id={"lat": partner})

    @pl.when(jnp.logical_not(has_peer))
    def _():
        greet(barrier)

    pl.semaphore_wait(barrier, jnp.where(has_peer, 2, 1 + beside))

    state = (even, odd, even)

    def pieces(s, g):
        cuts = 4 if s == STEPS - 1 and g == total - 1 else 1
        return [(g + c, c * (length // cuts), length // cuts) for c in range(cuts)]

    def chip_copy(s, g, piece):
        number, start, count = piece
        return pltpu.make_async_remote_copy(
            (tracer if s == 0 else state[s]).at[first, pl.ds(start, count), rows(g), :],
            chip.at[s, pl.ds(start, count), rows(g), :],
            chip_send.at[s, number],
            chip_recv.at[s, number],
            device_id={"lat": peer},
            device_id_type=MESH,
        )

    def pair_copy(s):
        return pltpu.make_async_remote_copy(
            (tracer if s == 0 else state[s]).at[plane(planes - 1)],
            pair.at[s],
            pair_send.at[s],
            pair_recv.at[s],
            device_id={"lat": partner},
            device_id_type=MESH,
        )

    def span(part):
        return pl.ds(rest, others) if part else pl.ds(first, 1)

    def k_copy(s, part, side):
        return pltpu.make_async_remote_copy(
            state[s].at[span(part), :, 0 if side else depth - 1, :],
            edge_k.at[s, side, span(part)],
            k_send.at[s, part, side],
            k_recv.at[s, part, side],
            device_id={"lev": lev - 1 if side else lev + 1},
            device_id_type=MESH,
        )

    def i_copy(s, part, side):
        return pltpu.make_async_remote_copy(
            state[s].at[span(part), 0 if side else length - 1],
            edge_i.at[s, side, span(part)],
            i_send.at[s, part, side],
            i_recv.at[s, part, side],
            device_id={"lon": lon - 1 if side else lon + 1},
            device_id_type=MESH,
        )

    def has(index, count, side):
        return index > 0 if side else index < count - 1

    def edges(action, s, part):
        for side in (0, 1):
            there = 1 - side if action == "wait_recv" else side

            @pl.when(has(lev, n_lev, there))
            def _(side=side):
                getattr(k_copy(s, part, side), action)()

            @pl.when(has(lon, n_lon, there))
            def _(side=side):
                getattr(i_copy(s, part, side), action)()

    def chip_all(action, s, which):
        @pl.when(has_peer)
        def _():
            for g in which:
                for piece in pieces(s, g):
                    getattr(chip_copy(s, g, piece), action)()

    chip_all("start", 0, groups)
    pair_copy(0).start()
    for n in range(3):
        for p in (*range(1, planes), 0):
            load(n, p).start()

    def clear(ref, count):
        def one(i, _):
            ref[i] = jnp.zeros(ref.shape[1:], jnp.float32)
            return _

        lax.fori_loop(0, count, one, 0)

    @pl.when(jnp.logical_not(has_peer))
    def _():
        for s in range(STEPS):
            clear(chip.at[s], length)

    for side in (0, 1):

        @pl.when(jnp.logical_not(has(lev, n_lev, 1 - side)))
        def _(side=side):
            for s in range(STEPS):
                clear(edge_k.at[s, side], planes)

        @pl.when(jnp.logical_not(has(lon, n_lon, 1 - side)))
        def _(side=side):
            for s in range(STEPS):
                clear(edge_i.at[s, side], planes)

    half = n_lat // 2
    low_half = lat < half
    depth_in = jnp.where(low_half, lat, n_lat - 1 - lat)
    inward = jnp.where(low_half, lat + 1, lat - 1)
    outward = jnp.where(low_half, lat - 1, lat + 1)

    @pl.when(depth_in < half - 1)
    def _():
        pl.semaphore_wait(gather, 1)

    @pl.when(depth_in > 0)
    def _():
        signal(gather, device_id={"lat": outward})
        pl.semaphore_wait(go, 1)

    @pl.when(depth_in == 0)
    def _():
        greet(across)
        pl.semaphore_wait(across, beside)

    @pl.when(depth_in < half - 1)
    def _():
        signal(go, device_id={"lat": inward})

    def loader(ref, *lead):
        return lambda i, g: ref[(*lead, i, rows(g), slice(None))]

    def advance(s, p, which, near, far, sums=None, start=0, count=length):
        j = plane(p)
        centre = loader(state[s], j)
        target = end if s == STEPS - 1 else state[s + 1]

        def store(i, g, value):
            target[j, i, rows(g), :] = value

        return sweep(
            start,
            count,
            which,
            total,
            centre,
            near,
            far,
            lambda base: edge_k[s, 0, j, pl.ds(base, ROWS), :],
            lambda base: edge_k[s, 1, j, pl.ds(base, ROWS), :],
            lambda g: centre(start - 1, g) if start else edge_i[s, 0, j, rows(g), :],
            lambda g: centre(start + count, g) if start + count < length else edge_i[s, 1, j, rows(g), :],
            loader(scaled, j),
            loader(end, j),
            store,
            sums,
        )

    def spread_of(j, which, sums, start, count):
        means = [v * (1.0 / count) for v in sums]

        def one(i, so_far):
            out = []
            for n, g in enumerate(which):
                d = end[j, start + i, rows(g), :] - means[n]
                out.append(so_far[n] + d * d)
            return out

        return means, along(count, one, nothing(which))

    def merged(one, other, start, count):
        (mean, squares), (mean_2, squares_2) = one, other
        off = mean_2 - mean
        share = count / (start + count)
        return mean + off * share, squares + squares_2 + off * off * (start * share)

    def combined(own, arrived):
        means = [own[0], *(a[0] for a in arrived)]
        mean = functools.reduce(jnp.add, means) * (1.0 / n_lon)
        off = functools.reduce(jnp.add, [(m - mean) * (m - mean) for m in means])
        squares = functools.reduce(jnp.add, [own[1], *(a[1] for a in arrived)])
        variance = (squares + off * float(length)) * (1.0 / (length * n_lon))
        return mean, lax.rsqrt(variance + 0.0001)

    def scale(j, which, pairs):
        def one(i, carry):
            for g, (mean, factor) in zip(which, pairs):
                scaled[j, i, rows(g), :] = (end[j, i, rows(g), :] - mean) * factor
            return carry

        along(length, one, 0)

    def sum_copy(r):
        return pltpu.make_async_remote_copy(
            mine,
            theirs.at[r - 1],
            sum_send.at[r - 1],
            sum_recv.at[r - 1],
            device_id={"lon": lax.rem(lon + r, n_lon)},
            device_id_type=MESH,
        )

    def sum_0_copy(r, g):
        return pltpu.make_async_remote_copy(
            mine_0.at[g],
            theirs_0.at[r - 1, g],
            sum_0_send.at[r - 1, g],
            sum_0_recv.at[r - 1, g],
            device_id={"lon": lax.rem(lon + r, n_lon)},
            device_id_type=MESH,
        )

    def nothing(which):
        return [jnp.zeros((ROWS, 128), jnp.float32) for _ in which]

    for p in range(planes):
        load(0, p).wait()
    for part in (1, 0):
        edges("start", 0, part)

    def scale_rest():
        for r in range(1, n_lon):
            sum_copy(r).wait_recv()
        for p in range(1, planes):
            pairs = []
            for g in groups:
                own = [mine[n, p - 1, rows(g), :] for n in (0, 1)]
                arrived = [[theirs[r, n, p - 1, rows(g), :] for n in (0, 1)] for r in range(n_lon - 1)]
                pairs.append(combined(own, arrived))
            scale(plane(p), groups, pairs)

    def line_0(g):
        for r in range(1, n_lon):
            sum_0_copy(r, g).wait_recv()
        arrived = [[theirs_0[r, g, n] for n in (0, 1)] for r in range(n_lon - 1)]
        return combined([mine_0[g, n] for n in (0, 1)], arrived)

    def scale_0(g):
        scale(first, [g], [line_0(g)])

    for s in range(STEPS):
        closing = s == STEPS - 1
        edges("wait_recv", s, 1)
        if s == 1:
            pair_copy(0).wait_send()
            for part in (1, 0):
                edges("wait_send", 0, part)
        for p in range(1, planes):
            j = plane(p)
            if s == 0:
                load(1, p).wait()
                load(2, p).wait()
            if p == planes - 1:
                pair_copy(s).wait_recv()
                far = loader(pair, s)
            else:
                far = loader(state[s], plane(p + 1))
            sums = advance(s, p, groups, loader(state[s], plane(p - 1)), far, nothing(groups) if closing else None)
            if closing:
                means, squares = spread_of(j, groups, sums, 0, length)
                for g in groups:
                    mine[0, p - 1, rows(g), :] = means[g]
                    mine[1, p - 1, rows(g), :] = squares[g]
        if closing:
            for r in range(1, n_lon):
                sum_copy(r).start()
        else:
            edges("start", s + 1, 1)
            pair_copy(s + 1).start()
        edges("wait_recv", s, 0)
        if s == 0:
            load(1, 0).wait()
            load(2, 0).wait()
        for g in groups:
            for piece in pieces(s, g):
                _, start, count = piece

                @pl.when(has_peer)
                def _(g=g, piece=piece):
                    chip_copy(s, g, piece).wait_recv()

                near, far = loader(chip, s), loader(state[s], plane(1))
                sums = advance(s, 0, [g], near, far, nothing([g]) if closing else None, start, count)
                if closing:
                    (mean,), (squares,) = spread_of(first, [g], sums, start, count)
                    line = merged(line, (mean, squares), start, count) if start else (mean, squares)
                if closing and g == total - 1 and start == 0:
                    scale_0(g - 1)
            if closing:
                for n in (0, 1):
                    mine_0[g, n] = line[n]
                for r in (*range(2, n_lon), 1):
                    sum_0_copy(r, g).start()
                if g == 0:
                    scale_rest()
                elif g < total - 1:
                    scale_0(g - 1)
                else:
                    for n, v in enumerate(line_0(g)):
                        closing_line[n] = v
            else:
                chip_all("start", s + 1, [g])
        if not closing:
            edges("start", s + 1, 0)

    for s in range(STEPS):
        chip_all("wait_send", s, groups)
    for s in range(1, STEPS):
        pair_copy(s).wait_send()
        for part in (1, 0):
            edges("wait_send", s, part)
    for r in range(1, n_lon):
        sum_copy(r).wait_send()
        for g in groups:
            sum_0_copy(r, g).wait_send()


def hand_out(scaled, end, line, scaled_out, end_out, last, sem):
    planes, length, depth, _ = end.shape
    core = lax.rem(lax.axis_index("lat"), 2)
    first, way = core * (planes - 1), 1 - 2 * core
    rows, held = pl.ds(depth - ROWS, ROWS), pl.ds(0, depth - ROWS)
    copies = [pltpu.make_async_copy(end.at[j], end_out.at[j], sem.at[0, j]) for j in range(planes)]
    for p in range(1, planes):
        j = first + way * p
        copies.append(pltpu.make_async_copy(scaled.at[j], scaled_out.at[j], sem.at[1, p]))
    copies.append(pltpu.make_async_copy(scaled.at[first, :, held], scaled_out.at[first, :, held], sem.at[1, 0]))
    for c in copies:
        c.start()
    mean, factor = line[0], line[1]

    def one(i, carry):
        last[i] = (end[first, i, rows, :] - mean) * factor
        return carry

    along(length, one, 0)
    copies.append(pltpu.make_async_copy(last, scaled_out.at[first, :, rows], sem.at[1, planes]))
    copies[-1].start()
    for c in copies:
        c.wait()


def shards(sizes, tracer, conductance, source):
    planes, length, depth, members = tracer.shape
    f32 = jnp.float32
    total = depth // ROWS
    lines = sizes[1] - 1
    dma = pltpu.SemaphoreType.DMA
    end, scaled, line = pl.pallas_call(
        functools.partial(march, sizes),
        out_shape=[pltpu.VMEM(a, f32) for a in (tracer.shape, tracer.shape, (2, ROWS, members))],
        in_specs=[pl.BlockSpec(memory_space=pltpu.HBM)] * 3,
        out_specs=[pl.BlockSpec(memory_space=pltpu.VMEM)] * 3,
        scratch_shapes=[
            pltpu.VMEM(tracer.shape, f32),
            pltpu.VMEM(tracer.shape, f32),
            pltpu.VMEM((STEPS, length, depth, members), f32),
            pltpu.VMEM((STEPS, length, depth, members), f32),
            pltpu.VMEM((STEPS, 2, planes, length, members), f32),
            pltpu.VMEM((STEPS, 2, planes, depth, members), f32),
            pltpu.VMEM((2, planes - 1, depth, members), f32),
            pltpu.VMEM((lines, 2, planes - 1, depth, members), f32),
            pltpu.VMEM((total, 2, ROWS, members), f32),
            pltpu.VMEM((lines, total, 2, ROWS, members), f32),
            pltpu.SemaphoreType.REGULAR,
            pltpu.SemaphoreType.REGULAR,
            pltpu.SemaphoreType.REGULAR,
            dma((3, planes)),
            dma((STEPS, total + 3)),
            dma((STEPS, total + 3)),
            dma((STEPS,)),
            dma((STEPS,)),
            dma((STEPS, 2, 2)),
            dma((STEPS, 2, 2)),
            dma((STEPS, 2, 2)),
            dma((STEPS, 2, 2)),
            dma((lines,)),
            dma((lines,)),
            dma((lines, total)),
            dma((lines, total)),
        ],
        compiler_params=pltpu.CompilerParams(
            collective_id=0, has_side_effects=True, vmem_limit_bytes=36 << 20
        ),
        name="march",
    )(tracer, conductance, source)
    scaled, end = pl.pallas_call(
        hand_out,
        out_shape=[jax.ShapeDtypeStruct(tracer.shape, f32)] * 2,
        in_specs=[pl.BlockSpec(memory_space=pltpu.VMEM)] * 3,
        out_specs=[pl.BlockSpec(memory_space=pltpu.HBM)] * 2,
        scratch_shapes=[pltpu.VMEM((length, ROWS, members), f32), dma((2, planes + 1))],
        compiler_params=pltpu.CompilerParams(vmem_limit_bytes=2 << 20),
        name="hand_out",
    )(scaled, end, line)
    return scaled, end


def solution(mesh):
    sizes = tuple(mesh.shape[a] for a in ("lat", "lon", "lev"))
    placed = P("lat", "lon", "lev", None)
    return jax.shard_map(
        functools.partial(shards, sizes),
        mesh=mesh,
        in_specs=(placed,) * 3,
        out_specs=(placed, placed),
        check_vma=False,
    )
```

```python
import functools

import jax
import jax.numpy as jnp
from jax import lax
from jax.experimental import pallas as pl
from jax.experimental.pallas import tpu as pltpu
from jax.sharding import PartitionSpec as P

STEPS = 3
ROWS = 8
MESH = pl.DeviceIdType.MESH


def sweep(start, length, groups, total, centre, near, far, low, high, before, after, held, added, store, sums):
    row = lax.broadcasted_iota(jnp.int32, (ROWS, 128), 0)
    first, last = row == 0, row == ROWS - 1

    def block(t, carry, closing):
        previous, current, so_far = carry
        base = start + t * ROWS if closing else pl.multiple_of(start + t * ROWS, ROWS)
        lows = low(base) if 0 in groups else None
        highs = high(base) if total - 1 in groups else None
        for q in range(ROWS):
            i = base + q
            if closing and q == ROWS - 1:
                following = [after(g) for g in groups]
            else:
                following = [centre(i + 1, g) for g in groups]
            row_of = dict(zip(groups, current))
            for g in (groups[0] - 1, groups[-1] + 1):
                if 0 <= g < total:
                    row_of[g] = centre(i, g)
            down = {g: pltpu.roll(v, 1, 0) for g, v in row_of.items() if g <= groups[-1]}
            up = {g: pltpu.roll(v, ROWS - 1, 0) for g, v in row_of.items() if g >= groups[0]}
            if lows is not None:
                down[-1] = jnp.broadcast_to(lows[q : q + 1], (ROWS, 128))
            if highs is not None:
                up[total] = jnp.broadcast_to(highs[q : q + 1], (ROWS, 128))
            done = []
            for n, g in enumerate(groups):
                lower = jnp.where(first, down[g - 1], down[g])
                upper = jnp.where(last, up[g + 1], up[g])
                spread = (lower + upper) + (previous[n] + following[n]) + (near(i, g) + far(i, g))
                spread = spread - 6.0 * current[n]
                value = current[n] + held(i, g) * spread + added(i, g)
                store(i, g, value)
                done.append(value)
            if sums is not None:
                so_far = [a + b for a, b in zip(so_far, done)]
            previous, current = current, following
        return previous, current, so_far

    carry = ([before(g) for g in groups], [centre(start, g) for g in groups], sums or [])
    blocks = length // ROWS
    carry = lax.fori_loop(0, blocks - 1, lambda t, c: block(t, c, False), carry)
    return block(blocks - 1, carry, True)[2]


def along(length, body, carry, unroll=8):
    def block(t, carry):
        for q in range(unroll):
            carry = body(t * unroll + q, carry)
        return carry

    return lax.fori_loop(0, length // unroll, block, carry)


def march(
    sizes,
    tracer,
    conductance,
    source,
    end,
    scaled,
    closing_line,
    even,
    odd,
    chip,
    pair,
    edge_k,
    edge_i,
    mine,
    theirs,
    mine_0,
    theirs_0,
    gather,
    across,
    go,
    load_sem,
    chip_send,
    chip_recv,
    pair_send,
    pair_recv,
    k_send,
    k_recv,
    i_send,
    i_recv,
    sum_send,
    sum_recv,
    sum_0_send,
    sum_0_recv,
):
    n_lat, n_lon, n_lev = sizes
    planes, length, depth, _ = tracer.shape
    groups = list(range(depth // ROWS))
    total = len(groups)
    lat, lon, lev = (lax.axis_index(a) for a in ("lat", "lon", "lev"))
    core = lax.rem(lat, 2)
    way = 1 - 2 * core
    first = core * (planes - 1)
    rest = 1 - core
    partner = lat + way
    peer = lat - way
    has_peer = jnp.logical_and(peer >= 0, peer < n_lat)
    others = planes - 1

    def plane(p):
        return first + way * p

    def rows(g):
        return pl.ds(ROWS * g, ROWS)

    def load(n, p):
        a, b = ((tracer, even), (conductance, scaled), (source, end))[n]
        return pltpu.make_async_copy(a.at[plane(p)], b.at[plane(p)], load_sem.at[n, p])


    barrier = pltpu.get_barrier_semaphore()
    signal = functools.partial(pl.semaphore_signal, inc=1, device_id_type=MESH)

    def greet(semaphore):
        for r in range(1, n_lon):
            signal(semaphore, device_id={"lon": lax.rem(lon + r, n_lon)})

        @pl.when(lev > 0)
        def _():
            signal(semaphore, device_id={"lev": lev - 1})

        @pl.when(lev < n_lev - 1)
        def _():
            signal(semaphore, device_id={"lev": lev + 1})

    beside = n_lon - 1 + (lev > 0).astype(jnp.int32) + (lev < n_lev - 1).astype(jnp.int32)

    @pl.when(has_peer)
    def _():
        signal(barrier, device_id={"lat": peer})

    signal(barrier, device_id={"lat": partner})

    @pl.when(jnp.logical_not(has_peer))
    def _():
        greet(barrier)

    pl.semaphore_wait(barrier, jnp.where(has_peer, 2, 1 + beside))

    state = (even, odd, even)

    def pieces(s, g):
        cuts = 4 if s == STEPS - 1 and g == total - 1 else 1
        return [(g + c, c * (length // cuts), length // cuts) for c in range(cuts)]

    def chip_copy(s, g, piece):
        number, start, count = piece
        return pltpu.make_async_remote_copy(
            (tracer if s == 0 else state[s]).at[first, pl.ds(start, count), rows(g), :],
            chip.at[s, pl.ds(start, count), rows(g), :],
            chip_send.at[s, number],
            chip_recv.at[s, number],
            device_id={"lat": peer},
            device_id_type=MESH,
        )

    def pair_copy(s):
        return pltpu.make_async_remote_copy(
            (tracer if s == 0 else state[s]).at[plane(planes - 1)],
            pair.at[s],
            pair_send.at[s],
            pair_recv.at[s],
            device_id={"lat": partner},
            device_id_type=MESH,
        )

    def span(part):
        return pl.ds(rest, others) if part else pl.ds(first, 1)

    def k_copy(s, part, side):
        return pltpu.make_async_remote_copy(
            state[s].at[span(part), :, 0 if side else depth - 1, :],
            edge_k.at[s, side, span(part)],
            k_send.at[s, part, side],
            k_recv.at[s, part, side],
            device_id={"lev": lev - 1 if side else lev + 1},
            device_id_type=MESH,
        )

    def i_copy(s, part, side):
        return pltpu.make_async_remote_copy(
            state[s].at[span(part), 0 if side else length - 1],
            edge_i.at[s, side, span(part)],
            i_send.at[s, part, side],
            i_recv.at[s, part, side],
            device_id={"lon": lon - 1 if side else lon + 1},
            device_id_type=MESH,
        )

    def has(index, count, side):
        return index > 0 if side else index < count - 1

    def edges(action, s, part):
        for side in (0, 1):
            there = 1 - side if action == "wait_recv" else side

            @pl.when(has(lev, n_lev, there))
            def _(side=side):
                getattr(k_copy(s, part, side), action)()

            @pl.when(has(lon, n_lon, there))
            def _(side=side):
                getattr(i_copy(s, part, side), action)()

    def chip_all(action, s, which):
        @pl.when(has_peer)
        def _():
            for g in which:
                for piece in pieces(s, g):
                    getattr(chip_copy(s, g, piece), action)()

    chip_all("start", 0, groups)
    pair_copy(0).start()
    for n in range(3):
        for p in (*range(1, planes), 0):
            load(n, p).start()

    def clear(ref, count):
        def one(i, _):
            ref[i] = jnp.zeros(ref.shape[1:], jnp.float32)
            return _

        lax.fori_loop(0, count, one, 0)

    @pl.when(jnp.logical_not(has_peer))
    def _():
        for s in range(STEPS):
            clear(chip.at[s], length)

    for side in (0, 1):

        @pl.when(jnp.logical_not(has(lev, n_lev, 1 - side)))
        def _(side=side):
            for s in range(STEPS):
                clear(edge_k.at[s, side], planes)

        @pl.when(jnp.logical_not(has(lon, n_lon, 1 - side)))
        def _(side=side):
            for s in range(STEPS):
                clear(edge_i.at[s, side], planes)

    half = n_lat // 2
    low_half = lat < half
    depth_in = jnp.where(low_half, lat, n_lat - 1 - lat)
    inward = jnp.where(low_half, lat + 1, lat - 1)
    outward = jnp.where(low_half, lat - 1, lat + 1)

    @pl.when(depth_in < half - 1)
    def _():
        pl.semaphore_wait(gather, 1)

    @pl.when(depth_in > 0)
    def _():
        signal(gather, device_id={"lat": outward})
        pl.semaphore_wait(go, 1)

    @pl.when(depth_in == 0)
    def _():
        greet(across)
        pl.semaphore_wait(across, beside)

    @pl.when(depth_in < half - 1)
    def _():
        signal(go, device_id={"lat": inward})

    def loader(ref, *lead):
        return lambda i, g: ref[(*lead, i, rows(g), slice(None))]

    def advance(s, p, which, near, far, sums=None, start=0, count=length):
        j = plane(p)
        centre = loader(state[s], j)
        target = end if s == STEPS - 1 else state[s + 1]

        def store(i, g, value):
            target[j, i, rows(g), :] = value

        return sweep(
            start,
            count,
            which,
            total,
            centre,
            near,
            far,
            lambda base: edge_k[s, 0, j, pl.ds(base, ROWS), :],
            lambda base: edge_k[s, 1, j, pl.ds(base, ROWS), :],
            lambda g: centre(start - 1, g) if start else edge_i[s, 0, j, rows(g), :],
            lambda g: centre(start + count, g) if start + count < length else edge_i[s, 1, j, rows(g), :],
            loader(scaled, j),
            loader(end, j),
            store,
            sums,
        )

    def spread_of(j, which, sums, start, count):
        means = [v * (1.0 / count) for v in sums]

        def one(i, so_far):
            out = []
            for n, g in enumerate(which):
                d = end[j, start + i, rows(g), :] - means[n]
                out.append(so_far[n] + d * d)
            return out

        return means, along(count, one, nothing(which))

    def merged(one, other, start, count):
        (mean, squares), (mean_2, squares_2) = one, other
        off = mean_2 - mean
        share = count / (start + count)
        return mean + off * share, squares + squares_2 + off * off * (start * share)

    def combined(own, arrived):
        means = [own[0], *(a[0] for a in arrived)]
        mean = functools.reduce(jnp.add, means) * (1.0 / n_lon)
        off = functools.reduce(jnp.add, [(m - mean) * (m - mean) for m in means])
        squares = functools.reduce(jnp.add, [own[1], *(a[1] for a in arrived)])
        variance = (squares + off * float(length)) * (1.0 / (length * n_lon))
        return mean, lax.rsqrt(variance + 0.0001)

    def scale(j, which, pairs):
        def one(i, carry):
            for g, (mean, factor) in zip(which, pairs):
                scaled[j, i, rows(g), :] = (end[j, i, rows(g), :] - mean) * factor
            return carry

        along(length, one, 0)

    def sum_copy(r):
        return pltpu.make_async_remote_copy(
            mine,
            theirs.at[r - 1],
            sum_send.at[r - 1],
            sum_recv.at[r - 1],
            device_id={"lon": lax.rem(lon + r, n_lon)},
            device_id_type=MESH,
        )

    def sum_0_copy(r, g):
        return pltpu.make_async_remote_copy(
            mine_0.at[g],
            theirs_0.at[r - 1, g],
            sum_0_send.at[r - 1, g],
            sum_0_recv.at[r - 1, g],
            device_id={"lon": lax.rem(lon + r, n_lon)},
            device_id_type=MESH,
        )

    def nothing(which):
        return [jnp.zeros((ROWS, 128), jnp.float32) for _ in which]

    for p in range(planes):
        load(0, p).wait()
    for part in (1, 0):
        edges("start", 0, part)

    def scale_rest():
        for r in range(1, n_lon):
            sum_copy(r).wait_recv()
        for p in range(1, planes):
            pairs = []
            for g in groups:
                own = [mine[n, p - 1, rows(g), :] for n in (0, 1)]
                arrived = [[theirs[r, n, p - 1, rows(g), :] for n in (0, 1)] for r in range(n_lon - 1)]
                pairs.append(combined(own, arrived))
            scale(plane(p), groups, pairs)

    def line_0(g):
        for r in range(1, n_lon):
            sum_0_copy(r, g).wait_recv()
        arrived = [[theirs_0[r, g, n] for n in (0, 1)] for r in range(n_lon - 1)]
        return combined([mine_0[g, n] for n in (0, 1)], arrived)

    def scale_0(g):
        scale(first, [g], [line_0(g)])

    def all_sent():
        for s in range(STEPS):
            chip_all("wait_send", s, groups)
        for s in range(1, STEPS):
            pair_copy(s).wait_send()
            for part in (1, 0):
                edges("wait_send", s, part)
        for r in range(1, n_lon):
            sum_copy(r).wait_send()
            for g in groups:
                sum_0_copy(r, g).wait_send()

    for s in range(STEPS):
        closing = s == STEPS - 1
        edges("wait_recv", s, 1)
        if s == 1:
            pair_copy(0).wait_send()
            for part in (1, 0):
                edges("wait_send", 0, part)
        for p in range(1, planes):
            j = plane(p)
            if s == 0:
                load(1, p).wait()
                load(2, p).wait()
            if p == planes - 1:
                pair_copy(s).wait_recv()
                far = loader(pair, s)
            else:
                far = loader(state[s], plane(p + 1))
            sums = advance(s, p, groups, loader(state[s], plane(p - 1)), far, nothing(groups) if closing else None)
            if closing:
                means, squares = spread_of(j, groups, sums, 0, length)
                for g in groups:
                    mine[0, p - 1, rows(g), :] = means[g]
                    mine[1, p - 1, rows(g), :] = squares[g]
        if closing:
            for r in range(1, n_lon):
                sum_copy(r).start()
        else:
            edges("start", s + 1, 1)
            pair_copy(s + 1).start()
        edges("wait_recv", s, 0)
        if s == 0:
            load(1, 0).wait()
            load(2, 0).wait()
        for g in groups:
            for piece in pieces(s, g):
                _, start, count = piece

                @pl.when(has_peer)
                def _(g=g, piece=piece):
                    chip_copy(s, g, piece).wait_recv()

                near, far = loader(chip, s), loader(state[s], plane(1))
                sums = advance(s, 0, [g], near, far, nothing([g]) if closing else None, start, count)
                if closing:
                    (mean,), (squares,) = spread_of(first, [g], sums, start, count)
                    line = merged(line, (mean, squares), start, count) if start else (mean, squares)
                if closing and g == total - 1 and start == 0:
                    scale_0(g - 1)
            if closing:
                for n in (0, 1):
                    mine_0[g, n] = line[n]
                for r in (*range(2, n_lon), 1):
                    sum_0_copy(r, g).start()
                if g == 0:
                    scale_rest()
                elif g < total - 1:
                    scale_0(g - 1)
                else:
                    all_sent()
                    for n, v in enumerate(line_0(g)):
                        closing_line[n] = v
            else:
                chip_all("start", s + 1, [g])
        if not closing:
            edges("start", s + 1, 0)


def hand_out(scaled, end, line, scaled_out, end_out, last, sem):
    planes, length, depth, _ = end.shape
    core = lax.rem(lax.axis_index("lat"), 2)
    first, way = core * (planes - 1), 1 - 2 * core
    rows, held = pl.ds(depth - ROWS, ROWS), pl.ds(0, depth - ROWS)
    copies = [pltpu.make_async_copy(end.at[j], end_out.at[j], sem.at[0, j]) for j in range(planes)]
    for p in range(1, planes):
        j = first + way * p
        copies.append(pltpu.make_async_copy(scaled.at[j], scaled_out.at[j], sem.at[1, p]))
    copies.append(pltpu.make_async_copy(scaled.at[first, :, held], scaled_out.at[first, :, held], sem.at[1, 0]))
    for c in copies:
        c.start()
    mean, factor = line[0], line[1]

    def one(i, carry):
        last[i] = (end[first, i, rows, :] - mean) * factor
        return carry

    along(length, one, 0)
    copies.append(pltpu.make_async_copy(last, scaled_out.at[first, :, rows], sem.at[1, planes]))
    copies[-1].start()
    for c in copies:
        c.wait()


def shards(sizes, tracer, conductance, source):
    planes, length, depth, members = tracer.shape
    f32 = jnp.float32
    total = depth // ROWS
    lines = sizes[1] - 1
    dma = pltpu.SemaphoreType.DMA
    end, scaled, line = pl.pallas_call(
        functools.partial(march, sizes),
        out_shape=[pltpu.VMEM(a, f32) for a in (tracer.shape, tracer.shape, (2, ROWS, members))],
        in_specs=[pl.BlockSpec(memory_space=pltpu.HBM)] * 3,
        out_specs=[pl.BlockSpec(memory_space=pltpu.VMEM)] * 3,
        scratch_shapes=[
            pltpu.VMEM(tracer.shape, f32),
            pltpu.VMEM(tracer.shape, f32),
            pltpu.VMEM((STEPS, length, depth, members), f32),
            pltpu.VMEM((STEPS, length, depth, members), f32),
            pltpu.VMEM((STEPS, 2, planes, length, members), f32),
            pltpu.VMEM((STEPS, 2, planes, depth, members), f32),
            pltpu.VMEM((2, planes - 1, depth, members), f32),
            pltpu.VMEM((lines, 2, planes - 1, depth, members), f32),
            pltpu.VMEM((total, 2, ROWS, members), f32),
            pltpu.VMEM((lines, total, 2, ROWS, members), f32),
            pltpu.SemaphoreType.REGULAR,
            pltpu.SemaphoreType.REGULAR,
            pltpu.SemaphoreType.REGULAR,
            dma((3, planes)),
            dma((STEPS, total + 3)),
            dma((STEPS, total + 3)),
            dma((STEPS,)),
            dma((STEPS,)),
            dma((STEPS, 2, 2)),
            dma((STEPS, 2, 2)),
            dma((STEPS, 2, 2)),
            dma((STEPS, 2, 2)),
            dma((lines,)),
            dma((lines,)),
            dma((lines, total)),
            dma((lines, total)),
        ],
        compiler_params=pltpu.CompilerParams(
            collective_id=0, has_side_effects=True, vmem_limit_bytes=36 << 20
        ),
        name="march",
    )(tracer, conductance, source)
    scaled, end = pl.pallas_call(
        hand_out,
        out_shape=[jax.ShapeDtypeStruct(tracer.shape, f32)] * 2,
        in_specs=[pl.BlockSpec(memory_space=pltpu.VMEM)] * 3,
        out_specs=[pl.BlockSpec(memory_space=pltpu.HBM)] * 2,
        scratch_shapes=[pltpu.VMEM((length, ROWS, members), f32), dma((2, planes + 1))],
        compiler_params=pltpu.CompilerParams(vmem_limit_bytes=2 << 20),
        name="hand_out",
    )(scaled, end, line)
    return scaled, end


def solution(mesh):
    sizes = tuple(mesh.shape[a] for a in ("lat", "lon", "lev"))
    placed = P("lat", "lon", "lev", None)
    return jax.shard_map(
        functools.partial(shards, sizes),
        mesh=mesh,
        in_specs=(placed,) * 3,
        out_specs=(placed, placed),
        check_vma=False,
    )
```

```python
import functools

import jax
import jax.numpy as jnp
from jax import lax
from jax.experimental import pallas as pl
from jax.experimental.pallas import tpu as pltpu
from jax.sharding import PartitionSpec as P

STEPS = 3
ROWS = 8
MESH = pl.DeviceIdType.MESH


def sweep(start, length, groups, total, centre, near, far, low, high, before, after, held, added, store, sums):
    row = lax.broadcasted_iota(jnp.int32, (ROWS, 128), 0)
    first, last = row == 0, row == ROWS - 1

    def block(t, carry, closing):
        previous, current, so_far = carry
        base = start + t * ROWS if closing else pl.multiple_of(start + t * ROWS, ROWS)
        lows = low(base) if 0 in groups else None
        highs = high(base) if total - 1 in groups else None
        for q in range(ROWS):
            i = base + q
            if closing and q == ROWS - 1:
                following = [after(g) for g in groups]
            else:
                following = [centre(i + 1, g) for g in groups]
            row_of = dict(zip(groups, current))
            for g in (groups[0] - 1, groups[-1] + 1):
                if 0 <= g < total:
                    row_of[g] = centre(i, g)
            down = {g: pltpu.roll(v, 1, 0) for g, v in row_of.items() if g <= groups[-1]}
            up = {g: pltpu.roll(v, ROWS - 1, 0) for g, v in row_of.items() if g >= groups[0]}
            if lows is not None:
                down[-1] = jnp.broadcast_to(lows[q : q + 1], (ROWS, 128))
            if highs is not None:
                up[total] = jnp.broadcast_to(highs[q : q + 1], (ROWS, 128))
            done = []
            for n, g in enumerate(groups):
                lower = jnp.where(first, down[g - 1], down[g])
                upper = jnp.where(last, up[g + 1], up[g])
                spread = (lower + upper) + (previous[n] + following[n]) + (near(i, g) + far(i, g))
                spread = spread - 6.0 * current[n]
                value = current[n] + held(i, g) * spread + added(i, g)
                store(i, g, value)
                done.append(value)
            if sums is not None:
                so_far = [a + b for a, b in zip(so_far, done)]
            previous, current = current, following
        return previous, current, so_far

    carry = ([before(g) for g in groups], [centre(start, g) for g in groups], sums or [])
    blocks = length // ROWS
    carry = lax.fori_loop(0, blocks - 1, lambda t, c: block(t, c, False), carry)
    return block(blocks - 1, carry, True)[2]


def along(length, body, carry, unroll=8):
    def block(t, carry):
        for q in range(unroll):
            carry = body(t * unroll + q, carry)
        return carry

    return lax.fori_loop(0, length // unroll, block, carry)


def march(
    sizes,
    tracer,
    conductance,
    source,
    end,
    scaled,
    closing_line,
    even,
    odd,
    chip,
    pair,
    edge_k,
    edge_i,
    mine,
    theirs,
    mine_0,
    theirs_0,
    gather,
    across,
    go,
    load_sem,
    chip_send,
    chip_recv,
    pair_send,
    pair_recv,
    k_send,
    k_recv,
    i_send,
    i_recv,
    sum_send,
    sum_recv,
    sum_0_send,
    sum_0_recv,
):
    n_lat, n_lon, n_lev = sizes
    planes, length, depth, _ = tracer.shape
    groups = list(range(depth // ROWS))
    total = len(groups)
    lat, lon, lev = (lax.axis_index(a) for a in ("lat", "lon", "lev"))
    core = lax.rem(lat, 2)
    way = 1 - 2 * core
    first = core * (planes - 1)
    rest = 1 - core
    partner = lat + way
    peer = lat - way
    has_peer = jnp.logical_and(peer >= 0, peer < n_lat)
    others = planes - 1

    def plane(p):
        return first + way * p

    def rows(g):
        return pl.ds(ROWS * g, ROWS)

    def load(n, p):
        a, b = ((tracer, even), (conductance, scaled), (source, end))[n]
        return pltpu.make_async_copy(a.at[plane(p)], b.at[plane(p)], load_sem.at[n, p])


    barrier = pltpu.get_barrier_semaphore()
    signal = functools.partial(pl.semaphore_signal, inc=1, device_id_type=MESH)

    def greet(semaphore):
        for r in range(1, n_lon):
            signal(semaphore, device_id={"lon": lax.rem(lon + r, n_lon)})

        @pl.when(lev > 0)
        def _():
            signal(semaphore, device_id={"lev": lev - 1})

        @pl.when(lev < n_lev - 1)
        def _():
            signal(semaphore, device_id={"lev": lev + 1})

    beside = n_lon - 1 + (lev > 0).astype(jnp.int32) + (lev < n_lev - 1).astype(jnp.int32)

    @pl.when(has_peer)
    def _():
        signal(barrier, device_id={"lat": peer})

    signal(barrier, device_id={"lat": partner})

    @pl.when(jnp.logical_not(has_peer))
    def _():
        greet(barrier)

    pl.semaphore_wait(barrier, jnp.where(has_peer, 2, 1 + beside))

    state = (even, odd, even)

    def pieces(s, g):
        cuts = 4 if s == STEPS - 1 and g == total - 1 else 1
        return [(g + c, c * (length // cuts), length // cuts) for c in range(cuts)]

    def units(s):
        size = 1 if s == STEPS - 1 else 2
        return [groups[n : n + size] for n in range(0, total, size)]

    def block(s, g):
        return pl.ds(ROWS * g, ROWS * len(units(s)[0]))

    def chip_copy(s, g, piece):
        number, start, count = piece
        return pltpu.make_async_remote_copy(
            (tracer if s == 0 else state[s]).at[first, pl.ds(start, count), block(s, g), :],
            chip.at[s, pl.ds(start, count), block(s, g), :],
            chip_send.at[s, number],
            chip_recv.at[s, number],
            device_id={"lat": peer},
            device_id_type=MESH,
        )

    def pair_copy(s):
        return pltpu.make_async_remote_copy(
            (tracer if s == 0 else state[s]).at[plane(planes - 1)],
            pair.at[s],
            pair_send.at[s],
            pair_recv.at[s],
            device_id={"lat": partner},
            device_id_type=MESH,
        )

    def span(part):
        return pl.ds(rest, others) if part else pl.ds(first, 1)

    def k_copy(s, part, side):
        return pltpu.make_async_remote_copy(
            state[s].at[span(part), :, 0 if side else depth - 1, :],
            edge_k.at[s, side, span(part)],
            k_send.at[s, part, side],
            k_recv.at[s, part, side],
            device_id={"lev": lev - 1 if side else lev + 1},
            device_id_type=MESH,
        )

    def i_copy(s, part, side):
        return pltpu.make_async_remote_copy(
            state[s].at[span(part), 0 if side else length - 1],
            edge_i.at[s, side, span(part)],
            i_send.at[s, part, side],
            i_recv.at[s, part, side],
            device_id={"lon": lon - 1 if side else lon + 1},
            device_id_type=MESH,
        )

    def has(index, count, side):
        return index > 0 if side else index < count - 1

    def edges(action, s, part):
        for side in (0, 1):
            there = 1 - side if action == "wait_recv" else side

            @pl.when(has(lev, n_lev, there))
            def _(side=side):
                getattr(k_copy(s, part, side), action)()

            @pl.when(has(lon, n_lon, there))
            def _(side=side):
                getattr(i_copy(s, part, side), action)()

    def chip_all(action, s, which):
        @pl.when(has_peer)
        def _():
            for g in which:
                for piece in pieces(s, g):
                    getattr(chip_copy(s, g, piece), action)()

    chip_all("start", 0, [u[0] for u in units(0)])
    pair_copy(0).start()
    for n in range(3):
        for p in (*range(1, planes), 0):
            load(n, p).start()

    def clear(ref, count):
        def one(i, _):
            ref[i] = jnp.zeros(ref.shape[1:], jnp.float32)
            return _

        lax.fori_loop(0, count, one, 0)

    @pl.when(jnp.logical_not(has_peer))
    def _():
        for s in range(STEPS):
            clear(chip.at[s], length)

    for side in (0, 1):

        @pl.when(jnp.logical_not(has(lev, n_lev, 1 - side)))
        def _(side=side):
            for s in range(STEPS):
                clear(edge_k.at[s, side], planes)

        @pl.when(jnp.logical_not(has(lon, n_lon, 1 - side)))
        def _(side=side):
            for s in range(STEPS):
                clear(edge_i.at[s, side], planes)

    half = n_lat // 2
    low_half = lat < half
    depth_in = jnp.where(low_half, lat, n_lat - 1 - lat)
    inward = jnp.where(low_half, lat + 1, lat - 1)
    outward = jnp.where(low_half, lat - 1, lat + 1)

    @pl.when(depth_in < half - 1)
    def _():
        pl.semaphore_wait(gather, 1)

    @pl.when(depth_in > 0)
    def _():
        signal(gather, device_id={"lat": outward})
        pl.semaphore_wait(go, 1)

    @pl.when(depth_in == 0)
    def _():
        greet(across)
        pl.semaphore_wait(across, beside)

    @pl.when(depth_in < half - 1)
    def _():
        signal(go, device_id={"lat": inward})

    def loader(ref, *lead):
        return lambda i, g: ref[(*lead, i, rows(g), slice(None))]

    def advance(s, p, which, near, far, sums=None, start=0, count=length):
        j = plane(p)
        centre = loader(state[s], j)
        target = end if s == STEPS - 1 else state[s + 1]

        def store(i, g, value):
            target[j, i, rows(g), :] = value

        return sweep(
            start,
            count,
            which,
            total,
            centre,
            near,
            far,
            lambda base: edge_k[s, 0, j, pl.ds(base, ROWS), :],
            lambda base: edge_k[s, 1, j, pl.ds(base, ROWS), :],
            lambda g: centre(start - 1, g) if start else edge_i[s, 0, j, rows(g), :],
            lambda g: centre(start + count, g) if start + count < length else edge_i[s, 1, j, rows(g), :],
            loader(scaled, j),
            loader(end, j),
            store,
            sums,
        )

    def spread_of(j, which, sums, start, count):
        means = [v * (1.0 / count) for v in sums]

        def one(i, so_far):
            out = []
            for n, g in enumerate(which):
                d = end[j, start + i, rows(g), :] - means[n]
                out.append(so_far[n] + d * d)
            return out

        return means, along(count, one, nothing(which))

    def merged(one, other, start, count):
        (mean, squares), (mean_2, squares_2) = one, other
        off = mean_2 - mean
        share = count / (start + count)
        return mean + off * share, squares + squares_2 + off * off * (start * share)

    def combined(own, arrived):
        means = [own[0], *(a[0] for a in arrived)]
        mean = functools.reduce(jnp.add, means) * (1.0 / n_lon)
        off = functools.reduce(jnp.add, [(m - mean) * (m - mean) for m in means])
        squares = functools.reduce(jnp.add, [own[1], *(a[1] for a in arrived)])
        variance = (squares + off * float(length)) * (1.0 / (length * n_lon))
        return mean, lax.rsqrt(variance + 0.0001)

    def scale(j, which, pairs):
        def one(i, carry):
            for g, (mean, factor) in zip(which, pairs):
                scaled[j, i, rows(g), :] = (end[j, i, rows(g), :] - mean) * factor
            return carry

        along(length, one, 0)

    def sum_copy(r):
        return pltpu.make_async_remote_copy(
            mine,
            theirs.at[r - 1],
            sum_send.at[r - 1],
            sum_recv.at[r - 1],
            device_id={"lon": lax.rem(lon + r, n_lon)},
            device_id_type=MESH,
        )

    def sum_0_copy(r, g):
        return pltpu.make_async_remote_copy(
            mine_0.at[g],
            theirs_0.at[r - 1, g],
            sum_0_send.at[r - 1, g],
            sum_0_recv.at[r - 1, g],
            device_id={"lon": lax.rem(lon + r, n_lon)},
            device_id_type=MESH,
        )

    def nothing(which):
        return [jnp.zeros((ROWS, 128), jnp.float32) for _ in which]

    for p in range(planes):
        load(0, p).wait()
    for part in (1, 0):
        edges("start", 0, part)

    def scale_rest():
        for r in range(1, n_lon):
            sum_copy(r).wait_recv()
        for p in range(1, planes):
            pairs = []
            for g in groups:
                own = [mine[n, p - 1, rows(g), :] for n in (0, 1)]
                arrived = [[theirs[r, n, p - 1, rows(g), :] for n in (0, 1)] for r in range(n_lon - 1)]
                pairs.append(combined(own, arrived))
            scale(plane(p), groups, pairs)

    def line_0(g):
        for r in range(1, n_lon):
            sum_0_copy(r, g).wait_recv()
        arrived = [[theirs_0[r, g, n] for n in (0, 1)] for r in range(n_lon - 1)]
        return combined([mine_0[g, n] for n in (0, 1)], arrived)

    def scale_0(g):
        scale(first, [g], [line_0(g)])

    def all_sent():
        for s in range(STEPS):
            chip_all("wait_send", s, [u[0] for u in units(s)])
        for s in range(1, STEPS):
            pair_copy(s).wait_send()
            for part in (1, 0):
                edges("wait_send", s, part)
        for r in range(1, n_lon):
            sum_copy(r).wait_send()
            for g in groups:
                sum_0_copy(r, g).wait_send()

    for s in range(STEPS):
        closing = s == STEPS - 1
        edges("wait_recv", s, 1)
        if s == 1:
            pair_copy(0).wait_send()
            for part in (1, 0):
                edges("wait_send", 0, part)
        for p in range(1, planes):
            j = plane(p)
            if s == 0:
                load(1, p).wait()
                load(2, p).wait()
            if p == planes - 1:
                pair_copy(s).wait_recv()
                far = loader(pair, s)
            else:
                far = loader(state[s], plane(p + 1))
            sums = advance(s, p, groups, loader(state[s], plane(p - 1)), far, nothing(groups) if closing else None)
            if closing:
                means, squares = spread_of(j, groups, sums, 0, length)
                for g in groups:
                    mine[0, p - 1, rows(g), :] = means[g]
                    mine[1, p - 1, rows(g), :] = squares[g]
        if closing:
            for r in range(1, n_lon):
                sum_copy(r).start()
        else:
            edges("start", s + 1, 1)
            pair_copy(s + 1).start()
        edges("wait_recv", s, 0)
        if s == 0:
            load(1, 0).wait()
            load(2, 0).wait()
        for unit in units(s):
            g = unit[0]
            for piece in pieces(s, g):
                _, start, count = piece

                @pl.when(has_peer)
                def _(g=g, piece=piece):
                    chip_copy(s, g, piece).wait_recv()

                near, far = loader(chip, s), loader(state[s], plane(1))
                sums = advance(s, 0, unit, near, far, nothing([g]) if closing else None, start, count)
                if closing:
                    (mean,), (squares,) = spread_of(first, [g], sums, start, count)
                    line = merged(line, (mean, squares), start, count) if start else (mean, squares)
                if closing and g == total - 1 and start == 0:
                    scale_0(g - 1)
            if closing:
                for n in (0, 1):
                    mine_0[g, n] = line[n]
                for r in (*range(2, n_lon), 1):
                    sum_0_copy(r, g).start()
                if g == 0:
                    scale_rest()
                elif g < total - 1:
                    scale_0(g - 1)
                else:
                    all_sent()
                    for n, v in enumerate(line_0(g)):
                        closing_line[n] = v
            else:
                chip_all("start", s + 1, [u[0] for u in units(s + 1) if u[0] in unit])
        if not closing:
            edges("start", s + 1, 0)


def hand_out(scaled, end, line, scaled_out, end_out, last, sem):
    planes, length, depth, _ = end.shape
    core = lax.rem(lax.axis_index("lat"), 2)
    first, way = core * (planes - 1), 1 - 2 * core
    rows, held = pl.ds(depth - ROWS, ROWS), pl.ds(0, depth - ROWS)
    copies = [pltpu.make_async_copy(end.at[j], end_out.at[j], sem.at[0, j]) for j in range(planes)]
    for p in range(1, planes):
        j = first + way * p
        copies.append(pltpu.make_async_copy(scaled.at[j], scaled_out.at[j], sem.at[1, p]))
    copies.append(pltpu.make_async_copy(scaled.at[first, :, held], scaled_out.at[first, :, held], sem.at[1, 0]))
    for c in copies:
        c.start()
    mean, factor = line[0], line[1]

    def one(i, carry):
        last[i] = (end[first, i, rows, :] - mean) * factor
        return carry

    along(length, one, 0)
    copies.append(pltpu.make_async_copy(last, scaled_out.at[first, :, rows], sem.at[1, planes]))
    copies[-1].start()
    for c in copies:
        c.wait()


def shards(sizes, tracer, conductance, source):
    planes, length, depth, members = tracer.shape
    f32 = jnp.float32
    total = depth // ROWS
    lines = sizes[1] - 1
    dma = pltpu.SemaphoreType.DMA
    end, scaled, line = pl.pallas_call(
        functools.partial(march, sizes),
        out_shape=[pltpu.VMEM(a, f32) for a in (tracer.shape, tracer.shape, (2, ROWS, members))],
        in_specs=[pl.BlockSpec(memory_space=pltpu.HBM)] * 3,
        out_specs=[pl.BlockSpec(memory_space=pltpu.VMEM)] * 3,
        scratch_shapes=[
            pltpu.VMEM(tracer.shape, f32),
            pltpu.VMEM(tracer.shape, f32),
            pltpu.VMEM((STEPS, length, depth, members), f32),
            pltpu.VMEM((STEPS, length, depth, members), f32),
            pltpu.VMEM((STEPS, 2, planes, length, members), f32),
            pltpu.VMEM((STEPS, 2, planes, depth, members), f32),
            pltpu.VMEM((2, planes - 1, depth, members), f32),
            pltpu.VMEM((lines, 2, planes - 1, depth, members), f32),
            pltpu.VMEM((total, 2, ROWS, members), f32),
            pltpu.VMEM((lines, total, 2, ROWS, members), f32),
            pltpu.SemaphoreType.REGULAR,
            pltpu.SemaphoreType.REGULAR,
            pltpu.SemaphoreType.REGULAR,
            dma((3, planes)),
            dma((STEPS, total + 3)),
            dma((STEPS, total + 3)),
            dma((STEPS,)),
            dma((STEPS,)),
            dma((STEPS, 2, 2)),
            dma((STEPS, 2, 2)),
            dma((STEPS, 2, 2)),
            dma((STEPS, 2, 2)),
            dma((lines,)),
            dma((lines,)),
            dma((lines, total)),
            dma((lines, total)),
        ],
        compiler_params=pltpu.CompilerParams(
            collective_id=0, has_side_effects=True, vmem_limit_bytes=36 << 20
        ),
        name="march",
    )(tracer, conductance, source)
    scaled, end = pl.pallas_call(
        hand_out,
        out_shape=[jax.ShapeDtypeStruct(tracer.shape, f32)] * 2,
        in_specs=[pl.BlockSpec(memory_space=pltpu.VMEM)] * 3,
        out_specs=[pl.BlockSpec(memory_space=pltpu.HBM)] * 2,
        scratch_shapes=[pltpu.VMEM((length, ROWS, members), f32), dma((2, planes + 1))],
        compiler_params=pltpu.CompilerParams(vmem_limit_bytes=2 << 20),
        name="hand_out",
    )(scaled, end, line)
    return scaled, end


def solution(mesh):
    sizes = tuple(mesh.shape[a] for a in ("lat", "lon", "lev"))
    placed = P("lat", "lon", "lev", None)
    return jax.shard_map(
        functools.partial(shards, sizes),
        mesh=mesh,
        in_specs=(placed,) * 3,
        out_specs=(placed, placed),
        check_vma=False,
    )
```
